128 devices in a mesh: ctx: 16 (over y, z), wt: 8 (over x, core).
Axes of the slice: x: 4, y: 4, z: 4, core: 2. Of those that a mesh axis runs over, the one named last changes fastest.
Arguments:
- frames: bfloat16 [1024, 1280], P('wt'), may hold values from -6 to 6
- span_source: int32 [64], P('wt'), may hold values from 0 to 7, as said below
- adapter_weight: bfloat16 [1280, 4096], P(None, 'ctx'), may hold values from -0.15625 to 0.15625
- adapter_bias: float32 [4096], P('ctx'), may hold values from -3 to 3
- norm_gain: float32 [4096], replicated, may hold values from 0.25 to 1.75
- qkv_weight: bfloat16 [4096, 3, 4096], P('wt', None, 'ctx'), may hold values from -0.09375 to 0.09375
- out_weight: bfloat16 [4096, 4096], P('ctx', 'wt'), may hold values from -0.125 to 0.125
- k_cache: bfloat16 [16, 2048, 4096], P('wt', 'ctx'), may hold values from -600 to 600
- v_cache: bfloat16 [16, 2048, 4096], P('wt', 'ctx'), may hold values from -12 to 12
- lengths: int32 [16], P('wt'), may hold values from 1 to 2048
Outputs:
- attn_out: bfloat16 [1024, 4096], P('wt', 'ctx')
- new_keys: bfloat16 [1024, 4096], P('wt', 'ctx')
- new_values: bfloat16 [1024, 4096], P('wt', 'ctx')
The draws below stay inside these ranges and needn't reach their ends.
Inputs may be any that keep to these rules, and one draw needn't show every extreme that they name: `span_source`: each aligned block of 8 entries is a permutation of 0 to 7.
All inputs are finite; a program needn't handle non-finite values.
Results may differ from the reference program's by a relative error of at most 0.02.
Values may be sent and summed in bfloat16 or wider, within the bound.
No kernel may reach another device: no remote copies, remote signals or barrier semaphores. Data moves between devices by JAX's collectives and lax.ppermute only.
A program may use at most 64 MiB of HBM per device.

```python
import jax
import jax.numpy as jnp
from jax import lax

D = 4096
HEADS = 32
HEAD = 128
AUDIO = 1280
NEW = 64
SPAN = 16
MEETINGS = 16
TOKENS = 1024
HIST = 2048
GROUP_SPANS = 8
SPANS = 64


def draw_span_source(key, part):
    groups = SPANS // GROUP_SPANS
    group_keys = jax.random.split(jax.random.fold_in(key, 11), groups)
    orders = jax.vmap(lambda single: jax.random.permutation(single, GROUP_SPANS))(group_keys)
    return orders.reshape(SPANS).astype(jnp.int32)


def draw_k_cache(key, part):
    base = jax.random.truncated_normal(jax.random.fold_in(key, 21), -6.0, 6.0, (MEETINGS, HIST, D), jnp.float32)
    return base.astype(jnp.bfloat16)


def plant(values, key, low, largest):
    shape = values.shape
    index_at = [jax.random.randint(jax.random.fold_in(key, axis), (), 0, shape[axis]) for axis in range(len(shape))]
    values = values.at[tuple(index_at)].set(low)
    longest = shape.index(max(shape))
    index_at[longest] = (index_at[longest] + 1) % shape[longest]
    return values.at[tuple(index_at)].set(largest)


def raised(result, key, source, target, blocks, factor):
    def block_of(dim):
        return (jnp.arange(result.shape[dim]) // (result.shape[dim] // blocks)).reshape((-1,) + (1,) * (result.ndim - 1 - dim))

    one_side = jax.random.permutation(key, blocks)[block_of(target)]
    second = (block_of(target) + blocks // 2) % blocks
    return jnp.where((block_of(source) == one_side) | (block_of(source) == second), factor * result, result)


def level_of(rng, dims, pieces, low, top_value):
    level, own = 1.0, jax.random.fold_in(rng, 6)
    for position, shards_of in pieces:
        steps = jnp.exp(jax.random.uniform(jax.random.fold_in(own, position), (shards_of,), jnp.float32, low / len(pieces), top_value / len(pieces)))
        level = level * jnp.repeat(steps, dims[position] // shards_of).reshape([-1 if axis == position else 1 for axis in range(len(dims))])
    return level


def scatter_about(key, dims, deviation, most, cuts=(), kind=jnp.bfloat16):
    loudness = level_of(key, dims, cuts, -0.22, 0.18) if cuts else 1.0
    result = jax.random.normal(key, dims, jnp.float32) * deviation * loudness
    return jnp.minimum(jnp.maximum(result, -most), most).astype(kind)


def gaussian_with(rng, shape, width, bound, shards, heavy, kind=jnp.bfloat16):
    result = width * jax.random.normal(rng, shape, jnp.float32)
    if shards:
        result = result * level_of(rng, shape, shards, -0.22, 0.18)
    return jnp.clip(raised(result, jax.random.fold_in(rng, 3), *heavy), -bound, bound).astype(kind)


def setup_inputs(seed: int = 0) -> dict:
    keys = jax.random.split(jax.random.key(seed), 11)
    frames = scatter_about(keys[0], (TOKENS, AUDIO), 1.0, 6.0, ((0, 8),))
    span_source = draw_span_source(jax.random.fold_in(keys[10], 71), 0)
    adapter_weight = scatter_about(keys[2], (AUDIO, D), AUDIO ** -0.5, 0.15625, ((1, 16),))
    adapter_bias = scatter_about(keys[3], (D,), 0.5, 3.0, ((0, 16),), jnp.float32)
    norm_gain = jnp.clip(1.0 + 0.15 * jax.random.normal(keys[4], (D,), jnp.float32), 0.25, 1.75)
    qkv_weight = scatter_about(keys[5], (D, 3, D), D ** -0.5, 0.09375, ((0, 8), (2, 16)))
    out_weight = gaussian_with(keys[6], (D, D), D ** -0.5, 0.125, ((0, 16), (1, 8)), (0, 1, 16, 2.0))
    k_cache = draw_k_cache(jax.random.fold_in(keys[10], 71), 0)
    v_cache = scatter_about(keys[8], (MEETINGS, HIST, D), 2.0, 12.0, ((0, 8), (1, 16)))
    lengths = plant(jax.random.randint(keys[9], (MEETINGS,), 1, HIST + 1), jax.random.fold_in(keys[9], 1), 1, HIST).astype(jnp.int32)
    return dict(frames=frames, span_source=span_source, adapter_weight=adapter_weight, adapter_bias=adapter_bias, norm_gain=norm_gain, qkv_weight=qkv_weight, out_weight=out_weight, k_cache=k_cache, v_cache=v_cache, lengths=lengths)


def rotate(values, positions):
    half = values.shape[-1] // 2
    freq = 10000.0 ** (-2.0 * jnp.arange(half, dtype=jnp.float32) / values.shape[-1])
    angle = positions.astype(jnp.float32)[:, None] * freq[None, :]
    cosine = jnp.cos(angle)[:, None, :]
    sine = jnp.sin(angle)[:, None, :]
    first = values[..., :half]
    second = values[..., half:]
    return jnp.concatenate([first * cosine - second * sine, second * cosine + first * sine], axis=-1)

def attend_one(inputs):
    query, keys_hist, vals_hist, keys_new, vals_new, length = inputs
    scale = HEAD ** (-0.5)
    query_wide = query.astype(jnp.float32)
    score_hist = jnp.einsum('thd,phd->htp', query_wide, keys_hist.astype(jnp.float32)) * scale
    score_new = jnp.einsum('thd,shd->hts', query_wide, keys_new.astype(jnp.float32)) * scale
    live = jnp.arange(HIST, dtype=jnp.int32) < length
    causal = jnp.arange(NEW, dtype=jnp.int32)[:, None] >= jnp.arange(NEW, dtype=jnp.int32)[None, :]
    scores = jnp.concatenate([jnp.where(live[None, None, :], score_hist, -jnp.inf), jnp.where(causal[None, :, :], score_new, -jnp.inf)], axis=-1)
    row_max = lax.optimization_barrier(jnp.max(scores, axis=-1, keepdims=True))
    weights = jnp.exp(scores - row_max)
    row_total = lax.optimization_barrier(jnp.sum(weights, axis=-1))
    rounded = lax.optimization_barrier(weights.astype(jnp.bfloat16)).astype(jnp.float32)
    values_all = jnp.concatenate([vals_hist, vals_new], axis=0).astype(jnp.float32)
    numerator = jnp.einsum('htp,phd->thd', rounded, values_all)
    return (numerator / jnp.transpose(row_total)[:, :, None]).astype(jnp.bfloat16)

def reference(frames, span_source, adapter_weight, adapter_bias, norm_gain, qkv_weight, out_weight, k_cache, v_cache, lengths):
    base = jnp.arange(SPANS, dtype=jnp.int32) // GROUP_SPANS * GROUP_SPANS
    source = (base + span_source).astype(jnp.int32)
    ordered = frames.reshape(SPANS, SPAN, AUDIO)[source].reshape(TOKENS, AUDIO)
    tokens_in = (jnp.dot(ordered, adapter_weight, preferred_element_type=jnp.float32) + adapter_bias).astype(jnp.bfloat16)
    wide = tokens_in.astype(jnp.float32)
    normed = (wide * lax.rsqrt(lax.optimization_barrier(jnp.mean(wide * wide, axis=-1, keepdims=True)) + 1e-06) * norm_gain).astype(jnp.bfloat16)
    projected = jnp.dot(normed, qkv_weight.reshape(D, 3 * D), preferred_element_type=jnp.float32).reshape(TOKENS, 3, HEADS, HEAD)
    positions = (lengths[:, None] + jnp.arange(NEW, dtype=jnp.int32)[None, :]).reshape(TOKENS)
    queries = rotate(projected[:, 0], positions).astype(jnp.bfloat16)
    new_keys = rotate(projected[:, 1], positions).astype(jnp.bfloat16)
    new_values = projected[:, 2].astype(jnp.bfloat16)
    attended = lax.map(attend_one, (queries.reshape(MEETINGS, NEW, HEADS, HEAD), k_cache.reshape(MEETINGS, HIST, HEADS, HEAD), v_cache.reshape(MEETINGS, HIST, HEADS, HEAD), new_keys.reshape(MEETINGS, NEW, HEADS, HEAD), new_values.reshape(MEETINGS, NEW, HEADS, HEAD), lengths))
    attn_out = jnp.dot(attended.reshape(TOKENS, D), out_weight, preferred_element_type=jnp.float32).astype(jnp.bfloat16)
    return (attn_out, new_keys.reshape(TOKENS, D), new_values.reshape(TOKENS, D))
```

```python
import jax
import jax.numpy as jnp
from jax import lax
from jax.experimental import pallas as pl
from jax.experimental.pallas import tpu as pltpu
from jax.sharding import PartitionSpec as P

HEAD = 128
SIDE = 4
FLOOR = -1e30

bf16 = jnp.bfloat16
f32 = jnp.float32


def y_shift(x, k):
    pairs = [
        (y * SIDE + z, ((y + k) % SIDE) * SIDE + z) for y in range(SIDE) for z in range(SIDE)
    ]
    return lax.ppermute(x, "ctx", pairs)


def z_shift(x, k):
    pairs = [
        (y * SIDE + z, y * SIDE + (z + k) % SIDE) for y in range(SIDE) for z in range(SIDE)
    ]
    return lax.ppermute(x, "ctx", pairs)


def x_shift(x, k):
    pairs = [(2 * i + c, 2 * ((i + k) % SIDE) + c) for i in range(SIDE) for c in range(2)]
    return lax.ppermute(x, "wt", pairs)


def other_core(x):
    return lax.ppermute(x, "wt", [(i, i ^ 1) for i in range(2 * SIDE)])


def swap_xy(x):
    def place(i, y, z, c):
        return (y * SIDE + z) * 2 * SIDE + 2 * i + c

    pairs = [
        (place(i, y, z, c), place(y, i, z, c))
        for i in range(SIDE)
        for y in range(SIDE)
        for z in range(SIDE)
        for c in range(2)
    ]
    return lax.ppermute(x, ("ctx", "wt"), pairs)


ORDER = (1, 3, 2)


def from_ring(x, shift):
    got = {k: shift(x, k) for k in ORDER}
    return [x, got[1], got[2], got[3]]


def over_x(x):
    other = other_core(x)
    mine = from_ring(x, x_shift)
    return [mine[0], other] + [p for k in (1, 2, 3) for p in (mine[k], other_core(mine[k]))]


VMEM = pl.BlockSpec(memory_space=pltpu.VMEM)
SMEM = pl.BlockSpec(memory_space=pltpu.SMEM)
ANY = pl.BlockSpec(memory_space=pl.ANY)


def kernel_call(body, ins, out_shape, name, scratch=()):
    specs = [s for s, _ in ins]
    single = not isinstance(out_shape, tuple)
    return pl.pallas_call(
        body,
        in_specs=specs,
        out_specs=VMEM if single else tuple(VMEM for _ in out_shape),
        out_shape=out_shape,
        scratch_shapes=list(scratch),
        name=name,
    )(*[a for _, a in ins])


def shape(dims, kind):
    return jax.ShapeDtypeStruct(dims, kind)


def matmul(a, b):
    return jnp.dot(a, b, preferred_element_type=f32)


def matmul_t(a, b):
    return lax.dot_general(a, b, (((1,), (1,)), ((), ())), preferred_element_type=f32)


def adapter_body(source, frames, weight, bias, out, ordered):
    spans = source.shape[0]
    rows = frames.shape[0] // spans
    for g in range(spans):
        start = pl.multiple_of(source[g] * rows, rows)
        ordered[g * rows : (g + 1) * rows, :] = frames[pl.ds(start, rows), :]
    out[...] = (matmul(ordered[...], weight[...]) + bias[...]).astype(bf16)


def spin(u, cosine, sine):
    return u * cosine + pltpu.roll(u, HEAD // 2, 1) * sine


def pieces_product(place, normed, weights, take):
    total = None
    for n, weight in enumerate(weights):
        shard = 2 * ((place[0] + SIDE - n // 2) % SIDE) + (place[1] + n) % 2
        w = take(weight)
        half = w.shape[0] // 2
        part = matmul(normed[2 * shard], w[:half]) + matmul(normed[2 * shard + 1], w[half:])
        total = part if total is None else total + part
    return total


def query_body(place, s0, s1, s2, s3, gain, cosine, sine, *rest):
    weights, (query, normed) = rest[:8], rest[8:]
    stacks = (s0, s1, s2, s3)
    rows = s0.shape[1]
    squares = jnp.zeros((rows, 1), f32)
    for stack in stacks:
        for k in range(SIDE):
            wide = stack[k].astype(f32)
            squares = squares + jnp.sum(wide * wide, axis=-1, keepdims=True)
    width = SIDE * SIDE * s0.shape[2]
    factor = lax.rsqrt(squares * (1.0 / width) + 1e-06)
    for j, stack in enumerate(stacks):
        for k in range(SIDE):
            block = SIDE * ((place[2] + SIDE - k) % SIDE) + (place[3] + SIDE - j) % SIDE
            normed[block] = (stack[k].astype(f32) * factor * gain[block]).astype(bf16)
    projected = pieces_product(place, normed, weights, lambda w: w[...])
    for h in range(projected.shape[1] // HEAD):
        cut = slice(h * HEAD, (h + 1) * HEAD)
        query[:, cut] = spin(projected[:, cut], cosine[...], sine[...]).astype(bf16)


def key_value_body(place, normed, cosine, sine, *rest):
    weights, (keys, values) = rest[:8], rest[8:]
    projected = pieces_product(place, normed, weights, lambda w: w[0])
    for h in range(projected.shape[1] // HEAD):
        cut = slice(h * HEAD, (h + 1) * HEAD)
        keys[:, cut] = spin(projected[:, cut], cosine[...], sine[...]).astype(bf16)
    values[...] = pieces_product(place, normed, weights, lambda w: w[1]).astype(bf16)


def split_in_three(x):
    high = x.astype(bf16)
    rest = x - high.astype(f32)
    middle = rest.astype(bf16)
    low = (rest - middle.astype(f32)).astype(bf16)
    return high, middle, low


def soft_part(query, keys, values, live, scale):
    scores = matmul_t(query, keys) * scale
    scores = jnp.where(live, scores, FLOOR)
    most = jnp.max(scores, axis=-1, keepdims=True)
    weights = jnp.where(live, jnp.exp(scores - most), 0.0)
    total = jnp.sum(weights, axis=-1, keepdims=True)
    some = total > 0.0
    safe = jnp.where(some, total, 1.0)
    numer = matmul(weights.astype(bf16), values)
    return numer / safe, jnp.where(some, most + jnp.log(safe), FLOOR)


def history_body(step, place, lengths, stack, k_cache, v_cache, out, keys, values, logs, sems):
    copies = []
    for k in range(SIDE):
        block = SIDE * ((place[2] + SIDE - k) % SIDE) + (place[3] + SIDE - step) % SIDE
        start = pl.multiple_of(block * 256, 256)
        pair = (
            pltpu.make_async_copy(k_cache.at[:, :, pl.ds(start, 256)], keys.at[k], sems.at[0, k]),
            pltpu.make_async_copy(v_cache.at[:, :, pl.ds(start, 256)], values.at[k], sems.at[1, k]),
        )
        for copy in pair:
            copy.start()
        copies.append(pair)
    meetings, held = keys.shape[1], keys.shape[2]
    rows = stack.shape[1]
    new = rows // meetings
    first = (place[2] * SIDE + place[3]) * held
    spot = first + lax.broadcasted_iota(jnp.int32, (new, held), 1)
    logs[...] = jnp.zeros_like(logs)
    for k in range(SIDE):
        for copy in copies[k]:
            copy.wait()
        for m in range(meetings):
            live = spot < lengths[m]
            for h in range(2):
                cut = slice(h * HEAD, (h + 1) * HEAD)
                mean, log = soft_part(
                    stack[k, m * new : (m + 1) * new, cut],
                    keys[k, m, :, cut],
                    values[k, m, :, cut],
                    live,
                    HEAD**-0.5,
                )
                at = (2 * k + h) * rows + m * new
                out[at : at + new, :] = mean.astype(bf16)
                logs[m * new : (m + 1) * new, 2 * k + h : 2 * k + h + 1] = log
    turned = jnp.transpose(logs[...])[: 2 * SIDE]
    base = 2 * SIDE * rows
    parts = split_in_three(turned)
    out[base : base + 32, :] = jnp.concatenate(
        [p.astype(f32) for p in parts] + [jnp.zeros_like(turned)], axis=0
    ).astype(bf16)


def mixing(logs):
    top = logs[0]
    for log in logs[1:]:
        top = jnp.maximum(top, log)
    shares = [jnp.exp(log - top) for log in logs]
    total = shares[0]
    for share in shares[1:]:
        total = total + share
    return [share / total for share in shares], top + jnp.log(total)


def turned_shares(shares, rows):
    count = shares[0].shape[0]
    used = count * len(shares)
    fill = [jnp.zeros((rows - used, shares[0].shape[1]), f32)] if rows > used else []
    return jnp.transpose(jnp.concatenate(shares + fill, axis=0))


def row_mix_body(p0, p1, p2, p3, own, o1, o2, o3):
    parts = (p0, p1, p2, p3)
    outs = (own, o1, o2, o3)
    rows = p0.shape[1]
    heads = 2 * SIDE
    base = heads * rows
    logs = []
    for p in parts:
        tail = p[base : base + 32, :].astype(f32)
        logs.append(tail[:heads] + tail[heads : 2 * heads] + tail[2 * heads : 3 * heads])
    shares, log = mixing(logs)
    columns = turned_shares(shares, rows)
    spread = [part.astype(f32) for part in split_in_three(log)]
    for h in range(heads):
        mixed = None
        for i, p in enumerate(parts):
            term = p[h * rows : (h + 1) * rows, :].astype(f32) * columns[:, i * heads + h : i * heads + h + 1]
            mixed = term if mixed is None else mixed + term
        outs[h // 2][(h % 2) * rows : (h % 2 + 1) * rows, :] = mixed.astype(bf16)
    for k in range(SIDE):
        cut = slice(2 * k, 2 * k + 2)
        outs[k][2 * rows : 2 * rows + 16, :] = jnp.concatenate(
            [s[cut] for s in spread] + [jnp.zeros((10, rows), f32)], axis=0
        ).astype(bf16)


def new_part_body(query, keys, values, means, logs_out, logs):
    rows = query.shape[0]
    new = rows // 2
    causal = lax.broadcasted_iota(jnp.int32, (new, new), 0) >= lax.broadcasted_iota(
        jnp.int32, (new, new), 1
    )
    logs[...] = jnp.zeros_like(logs)
    for m in range(2):
        here = slice(m * new, (m + 1) * new)
        for h in range(2):
            cut = slice(h * HEAD, (h + 1) * HEAD)
            mean, log = soft_part(
                query[here, cut], keys[here, cut], values[here, cut], causal, HEAD**-0.5
            )
            means[h * rows + m * new : h * rows + (m + 1) * new, :] = mean
            logs[here, h : h + 1] = log
    logs_out[...] = jnp.transpose(logs[...])[:8]


def final_mix_body(p0, p1, p2, p3, means, new_logs, out):
    parts = (p0, p1, p2, p3)
    rows = means.shape[0] // 2
    logs = []
    for p in parts:
        tail = p[2 * rows : 2 * rows + 16, :].astype(f32)
        logs.append(tail[0:2] + tail[2:4] + tail[4:6])
    logs.append(new_logs[0:2])
    shares, _ = mixing(logs)
    columns = turned_shares(shares, rows)
    for h in range(2):
        cut = slice(h * rows, (h + 1) * rows)
        mixed = means[cut, :] * columns[:, 8 + h : 9 + h]
        for i, p in enumerate(parts):
            mixed = mixed + p[cut, :].astype(f32) * columns[:, 2 * i + h : 2 * i + h + 1]
        out[:, h * HEAD : (h + 1) * HEAD] = mixed.astype(bf16)


def project_body(place, a0, a1, a2, a3, *rest):
    weights, (own, o1, o2, o3, held, sums) = rest[:8], rest[8:]
    for k, a in enumerate((a0, a1, a2, a3)):
        held[(place[2] + SIDE - k) % SIDE] = a[...]
    for c in range(2):
        total = None
        for j in range(SIDE):
            part = matmul(held[(place[0] + SIDE - j) % SIDE], weights[2 * j + c][...])
            total = part if total is None else total + part
        first = 2 * ((place[1] + c) % 2)
        sums[first] = total[:, :256]
        sums[first + 1] = total[:, 256:]
    own[...] = sums[place[3]]
    for j, o in enumerate((o1, o2, o3)):
        o[...] = sums[(place[3] + j + 1) % SIDE].astype(bf16)


def shards(
    frames,
    span_source,
    adapter_weight,
    adapter_bias,
    norm_gain,
    qkv_weight,
    out_weight,
    k_cache,
    v_cache,
    lengths,
):
    rows = frames.shape[0]
    cols = adapter_weight.shape[1]
    meetings = lengths.shape[0]
    new = rows // meetings
    ctx_rank = lax.axis_index("ctx")
    wt_rank = lax.axis_index("wt")
    place = jnp.stack(
        [wt_rank // 2, wt_rank % 2, ctx_rank // SIDE, ctx_rank % SIDE]
    ).astype(jnp.int32)

    positions = (lengths[:, None] + jnp.arange(new, dtype=jnp.int32)[None, :]).reshape(rows)
    half = HEAD // 2
    freq = 10000.0 ** (-2.0 * jnp.arange(half, dtype=f32) / HEAD)
    angle = positions.astype(f32)[:, None] * freq[None, :]
    cosine = jnp.cos(angle)
    sine = jnp.sin(angle)
    cosine = jnp.concatenate([cosine, cosine], axis=-1)
    sine = jnp.concatenate([-sine, sine], axis=-1)

    adapted = kernel_call(
        adapter_body,
        [
            (SMEM, span_source),
            (VMEM, frames),
            (VMEM, adapter_weight),
            (VMEM, adapter_bias.reshape(1, cols)),
        ],
        shape((rows, cols), bf16),
        "adapter",
        [pltpu.VMEM(frames.shape, bf16)],
    )
    column = jnp.stack(from_ring(adapted, y_shift))
    stacks = from_ring(column, z_shift)

    by_kind = jnp.transpose(qkv_weight, (1, 0, 2))
    query_weights = over_x(by_kind[0])
    other_weights = over_x(by_kind[1:])
    out_weights = over_x(swap_xy(out_weight))

    gain = norm_gain.reshape(SIDE * SIDE, 1, cols)
    query, normed = kernel_call(
        query_body,
        [(SMEM, place)]
        + [(VMEM, s) for s in stacks]
        + [(VMEM, gain), (VMEM, cosine), (VMEM, sine)]
        + [(VMEM, w) for w in query_weights],
        (shape((rows, cols), bf16), shape((SIDE * SIDE, rows, cols), bf16)),
        "query",
    )
    query_stacks = from_ring(jnp.stack(from_ring(query, y_shift)), z_shift)

    keys, values = kernel_call(
        key_value_body,
        [(SMEM, place), (VMEM, normed), (VMEM, cosine), (VMEM, sine)]
        + [(VMEM, w) for w in other_weights],
        (shape((rows, cols), bf16), shape((rows, cols), bf16)),
        "key_value",
    )

    def history(step):
        held = k_cache.shape[1]
        return kernel_call(
            lambda *refs: history_body(step, *refs),
            [
                (SMEM, place),
                (SMEM, lengths),
                (VMEM, query_stacks[step]),
                (ANY, k_cache),
                (ANY, v_cache),
            ],
            shape((2 * SIDE * rows + 32, HEAD), bf16),
            f"history{step}",
            [
                pltpu.VMEM((SIDE, meetings, held, cols), bf16),
                pltpu.VMEM((SIDE, meetings, held, cols), bf16),
                pltpu.VMEM((rows, HEAD), f32),
                pltpu.SemaphoreType.DMA((2, SIDE)),
            ],
        )

    own = history(0)
    back = {j: z_shift(history(j), -j) for j in ORDER}
    block = shape((2 * rows + 16, HEAD), bf16)
    mixed = kernel_call(
        row_mix_body,
        [(VMEM, p) for p in (own, back[1], back[2], back[3])],
        (block, block, block, block),
        "row_mix",
    )
    returned = {k: y_shift(mixed[k], -k) for k in ORDER}
    means, new_logs = kernel_call(
        new_part_body,
        [(VMEM, query), (VMEM, keys), (VMEM, values)],
        (shape((2 * rows, HEAD), f32), shape((8, rows), f32)),
        "new_part",
        [pltpu.VMEM((rows, HEAD), f32)],
    )
    attended = kernel_call(
        final_mix_body,
        [(VMEM, p) for p in (mixed[0], returned[1], returned[2], returned[3], means, new_logs)],
        shape((rows, cols), bf16),
        "final_mix",
    )
    across = from_ring(attended, y_shift)
    part = shape((rows, cols), bf16)
    sums = kernel_call(
        project_body,
        [(SMEM, place)] + [(VMEM, a) for a in across] + [(VMEM, w) for w in out_weights],
        (shape((rows, cols), f32), part, part, part),
        "project",
        [pltpu.VMEM((SIDE, rows, cols), bf16), pltpu.VMEM((SIDE, rows, cols), f32)],
    )
    got = [z_shift(sums[j], j).astype(f32) for j in ORDER]
    attn_out = (sums[0] + got[0] + got[1] + got[2]).astype(bf16)
    return attn_out, keys, values


def solution(mesh):
    return jax.shard_map(
        shards,
        mesh=mesh,
        in_specs=(
            P("wt", None),
            P("wt"),
            P(None, "ctx"),
            P("ctx"),
            P(),
            P("wt", None, "ctx"),
            P("ctx", "wt"),
            P("wt", "ctx", None),
            P("wt", "ctx", None),
            P("wt"),
        ),
        out_specs=(P("wt", "ctx"), P("wt", "ctx"), P("wt", "ctx")),
        check_vma=False,
    )
```

```python
import jax
import jax.numpy as jnp
from jax import lax
from jax.experimental import pallas as pl
from jax.experimental.pallas import tpu as pltpu
from jax.sharding import PartitionSpec as P


HEAD = 128
SIDE = 4
FLOOR = -1e30

bf16 = jnp.bfloat16
f32 = jnp.float32


def y_shift(x, k):
    pairs = [
        (y * SIDE + z, ((y + k) % SIDE) * SIDE + z) for y in range(SIDE) for z in range(SIDE)
    ]
    return lax.ppermute(x, "ctx", pairs)


def z_shift(x, k):
    pairs = [
        (y * SIDE + z, y * SIDE + (z + k) % SIDE) for y in range(SIDE) for z in range(SIDE)
    ]
    return lax.ppermute(x, "ctx", pairs)


def x_shift(x, k):
    pairs = [(2 * i + c, 2 * ((i + k) % SIDE) + c) for i in range(SIDE) for c in range(2)]
    return lax.ppermute(x, "wt", pairs)


def other_core(x):
    return lax.ppermute(x, "wt", [(i, i ^ 1) for i in range(2 * SIDE)])


def swap_xy(x):
    def place(i, y, z, c):
        return (y * SIDE + z) * 2 * SIDE + 2 * i + c

    pairs = [
        (place(i, y, z, c), place(y, i, z, c))
        for i in range(SIDE)
        for y in range(SIDE)
        for z in range(SIDE)
        for c in range(2)
    ]
    return lax.ppermute(x, ("ctx", "wt"), pairs)


ORDER = (1, 3, 2)


def from_ring(x, shift):
    got = {k: shift(x, k) for k in ORDER}
    return [x, got[1], got[2], got[3]]


def over_x(x):
    mine = from_ring(x, x_shift)
    return [p for m in mine for p in (m, other_core(m))]


VMEM = pl.BlockSpec(memory_space=pltpu.VMEM)
SMEM = pl.BlockSpec(memory_space=pltpu.SMEM)
ANY = pl.BlockSpec(memory_space=pl.ANY)


def held(x):
    return pltpu.with_memory_space_constraint(x, pltpu.VMEM)


def kernel_call(body, ins, out_shape, scratch=(), limit=12):
    single = not isinstance(out_shape, tuple)
    return pl.pallas_call(
        body,
        in_specs=[s for s, _ in ins],
        out_specs=VMEM if single else tuple(VMEM for _ in out_shape),
        out_shape=out_shape,
        scratch_shapes=list(scratch),
        compiler_params=pltpu.CompilerParams(vmem_limit_bytes=limit << 20),
    )(*[held(a) if s is VMEM else a for s, a in ins])


def near(dims, kind):
    return pltpu.VMEM(dims, kind)


def far(dims, kind):
    return jax.ShapeDtypeStruct(dims, kind)


def matmul(a, b):
    return jnp.dot(a, b, preferred_element_type=f32)


def matmul_t(a, b):
    return lax.dot_general(a, b, (((1,), (1,)), ((), ())), preferred_element_type=f32)


def adapter_body(source, frames, weight, bias, kinds, out, query_weight, other_weight, ordered, sems):
    copies = (
        pltpu.make_async_copy(kinds.at[0], query_weight, sems.at[0]),
        pltpu.make_async_copy(kinds.at[1:3], other_weight, sems.at[1]),
    )
    for copy in copies:
        copy.start()
    spans = source.shape[0]
    rows = frames.shape[0] // spans
    for g in range(spans):
        start = pl.multiple_of(source[g] * rows, rows)
        ordered[g * rows : (g + 1) * rows, :] = frames[pl.ds(start, rows), :]
    out[...] = (matmul(ordered[...], weight[...]) + bias[...]).astype(bf16)
    for copy in copies:
        copy.wait()


def stack_body(a0, a1, a2, a3, out):
    for k, a in enumerate((a0, a1, a2, a3)):
        out[k] = a[...]


def stacked(parts):
    dims = (SIDE, *parts[0].shape)
    return kernel_call(stack_body, [(VMEM, p) for p in parts], near(dims, bf16))


def spin(u, cosine, sine):
    return u * cosine + pltpu.roll(u, HEAD // 2, 1) * sine


def pieces_product(place, normed, weights, take):
    total = None
    for n, weight in enumerate(weights):
        shard = 2 * ((place[0] + SIDE - n // 2) % SIDE) + (place[1] + n) % 2
        w = take(weight)
        half = w.shape[0] // 2
        part = matmul(normed[2 * shard], w[:half]) + matmul(normed[2 * shard + 1], w[half:])
        total = part if total is None else total + part
    return total


def query_body(place, s0, s1, s2, s3, gain, cosine, sine, *rest):
    weights, (query, normed) = rest[:8], rest[8:]
    stacks = (s0, s1, s2, s3)
    rows = s0.shape[1]
    sums = jnp.zeros((rows, HEAD), f32)
    for stack in stacks:
        for k in range(SIDE):
            wide = stack[k].astype(f32)
            square = wide * wide
            sums = sums + (square[:, :HEAD] + square[:, HEAD:])
    width = SIDE * SIDE * s0.shape[2]
    factor = lax.rsqrt(jnp.sum(sums, axis=-1, keepdims=True) * (1.0 / width) + 1e-06)
    for j, stack in enumerate(stacks):
        for k in range(SIDE):
            block = SIDE * ((place[2] + SIDE - k) % SIDE) + (place[3] + SIDE - j) % SIDE
            normed[block] = (stack[k].astype(f32) * factor * gain[block]).astype(bf16)
    projected = pieces_product(place, normed, weights, lambda w: w[...])
    for h in range(projected.shape[1] // HEAD):
        cut = slice(h * HEAD, (h + 1) * HEAD)
        query[:, cut] = spin(projected[:, cut], cosine[...], sine[...]).astype(bf16)


def key_value_body(place, normed, cosine, sine, *rest):
    weights, (keys, values) = rest[:8], rest[8:]
    projected = pieces_product(place, normed, weights, lambda w: w[0])
    for h in range(projected.shape[1] // HEAD):
        cut = slice(h * HEAD, (h + 1) * HEAD)
        keys[:, cut] = spin(projected[:, cut], cosine[...], sine[...]).astype(bf16)
    values[...] = pieces_product(place, normed, weights, lambda w: w[1]).astype(bf16)


def split_in_three(x):
    high = x.astype(bf16).astype(f32)
    middle = (x - high).astype(bf16).astype(f32)
    return high, middle, x - high - middle


def soft_weights(scores, live):
    scores = jnp.where(live, scores, FLOOR)
    most = jnp.max(scores, axis=-1, keepdims=True)
    weights = jnp.where(live, jnp.exp(scores - most), 0.0)
    return weights, most, jnp.sum(weights, axis=-1, keepdims=True)


def history_body(step, place, lengths, stack, k_cache, v_cache, out, scores, weights):
    meetings, span = k_cache.shape[0], k_cache.shape[1]
    rows = stack.shape[1]
    new = rows // meetings
    heads = 2 * SIDE
    starts = []
    for k in range(SIDE):
        block = SIDE * ((place[2] + SIDE - k) % SIDE) + (place[3] + SIDE - step) % SIDE
        for h in range(2):
            starts.append(pl.multiple_of(block * 256 + h * HEAD, HEAD))
    for i, start in enumerate(starts):
        cut = slice(i % 2 * HEAD, (i % 2 + 1) * HEAD)
        for m in range(meetings):
            here = slice(m * new, (m + 1) * new)
            scores[i, here, :] = matmul_t(
                stack[i // 2, here, cut], k_cache[m, :, pl.ds(start, HEAD)]
            )
    first = (place[2] * SIDE + place[3]) * span
    spot = first + lax.broadcasted_iota(jnp.int32, (rows, span), 1)
    upper = lax.broadcasted_iota(jnp.int32, (rows, span), 0) < new
    live = spot < jnp.where(upper, lengths[0], lengths[1])
    lane = lax.broadcasted_iota(jnp.int32, (rows, HEAD), 1)
    stats = jnp.zeros((rows, HEAD), f32)
    for i in range(heads):
        weight, most, total = soft_weights(scores[i] * HEAD**-0.5, live)
        weights[i] = weight.astype(bf16)
        stats = jnp.where(lane == i, most, jnp.where(lane == heads + i, total, stats))
    for i, start in enumerate(starts):
        for m in range(meetings):
            here = slice(m * new, (m + 1) * new)
            at = i * rows + m * new
            out[at : at + new, :] = matmul(
                weights[i, here, :], v_cache[m, :, pl.ds(start, HEAD)]
            ).astype(bf16)
    turned = jnp.transpose(stats)[: 2 * heads]
    base = heads * rows
    for n, piece in enumerate(split_in_three(turned)):
        out[base + 16 * n : base + 16 * n + 16, :] = piece.astype(bf16)


def turned_columns(pieces, rows):
    used = sum(p.shape[0] for p in pieces)
    fill = [jnp.zeros((rows - used, pieces[0].shape[1]), f32)] if rows > used else []
    return jnp.transpose(jnp.concatenate(list(pieces) + fill, axis=0))


def row_mix_body(p0, p1, p2, p3, own, o1, o2, o3):
    parts = (p0, p1, p2, p3)
    outs = (own, o1, o2, o3)
    heads = 2 * SIDE
    rows = p0.shape[1]
    base = heads * rows
    tops, totals = [], []
    for p in parts:
        tail = p[base : base + 48, :].astype(f32)
        stats = tail[:16] + tail[16:32] + tail[32:]
        tops.append(stats[:heads])
        totals.append(stats[heads:])
    top = jnp.maximum(jnp.maximum(tops[0], tops[1]), jnp.maximum(tops[2], tops[3]))
    factors = [jnp.exp(t - top) for t in tops]
    total = sum(t * f for t, f in zip(totals, factors))
    columns = turned_columns(factors, rows)
    for h in range(heads):
        cut = slice(h * rows, (h + 1) * rows)
        mixed = None
        for i, p in enumerate(parts):
            at = i * heads + h
            term = p[cut, :].astype(f32) * columns[:, at : at + 1]
            mixed = term if mixed is None else mixed + term
        outs[h // 2][(h % 2) * rows : (h % 2 + 1) * rows, :] = mixed.astype(bf16)
    spread = [piece for pair in zip(split_in_three(top), split_in_three(total)) for piece in pair]
    for k in range(SIDE):
        cut = slice(2 * k, 2 * k + 2)
        outs[k][2 * rows : 2 * rows + 16, :] = jnp.concatenate(
            [piece[cut] for piece in spread] + [jnp.zeros((4, rows), f32)], axis=0
        ).astype(bf16)


def new_part_body(query, keys, values, numer, stats_out):
    rows = query.shape[0]
    new = rows // 2
    causal = lax.broadcasted_iota(jnp.int32, (new, new), 0) >= lax.broadcasted_iota(
        jnp.int32, (new, new), 1
    )
    lane = lax.broadcasted_iota(jnp.int32, (new, HEAD), 1)
    stats = []
    for m in range(2):
        here = slice(m * new, (m + 1) * new)
        tile = jnp.zeros((new, HEAD), f32)
        for h in range(2):
            cut = slice(h * HEAD, (h + 1) * HEAD)
            weight, most, total = soft_weights(
                matmul_t(query[here, cut], keys[here, cut]) * HEAD**-0.5, causal
            )
            numer[h * rows + m * new : h * rows + (m + 1) * new, :] = matmul(
                weight.astype(bf16), values[here, cut]
            )
            tile = jnp.where(lane == h, most, jnp.where(lane == 2 + h, total, tile))
        stats.append(tile)
    stats_out[...] = jnp.transpose(jnp.concatenate(stats, axis=0))[:8]


def final_mix_body(p0, p1, p2, p3, numer, new_stats, out):
    parts = (p0, p1, p2, p3)
    rows = numer.shape[0] // 2
    tops, totals = [], []
    for p in parts:
        tail = p[2 * rows : 2 * rows + 16, :].astype(f32)
        tops.append(tail[0:2] + tail[4:6] + tail[8:10])
        totals.append(tail[2:4] + tail[6:8] + tail[10:12])
    tops.append(new_stats[0:2])
    totals.append(new_stats[2:4])
    top = tops[0]
    for t in tops[1:]:
        top = jnp.maximum(top, t)
    factors = [jnp.exp(t - top) for t in tops]
    total = sum(t * f for t, f in zip(totals, factors))
    columns = turned_columns([f / total for f in factors], rows)
    for h in range(2):
        cut = slice(h * rows, (h + 1) * rows)
        mixed = numer[cut, :] * columns[:, 8 + h : 9 + h]
        for i, p in enumerate(parts):
            mixed = mixed + p[cut, :].astype(f32) * columns[:, 2 * i + h : 2 * i + h + 1]
        out[:, h * HEAD : (h + 1) * HEAD] = mixed.astype(bf16)


def project_body(place, a0, a1, a2, a3, *rest):
    weights, (own, o1, o2, o3, across, sums) = rest[:8], rest[8:]
    for k, a in enumerate((a0, a1, a2, a3)):
        across[(place[2] + SIDE - k) % SIDE] = a[...]
    for c in range(2):
        total = None
        for j in range(SIDE):
            part = matmul(across[(place[0] + SIDE - j) % SIDE], weights[2 * j + c][...])
            total = part if total is None else total + part
        first = 2 * ((place[1] + c) % 2)
        sums[first] = total[:, :256]
        sums[first + 1] = total[:, 256:]
    own[...] = sums[place[3]]
    for j, o in enumerate((o1, o2, o3)):
        o[...] = sums[(place[3] + j + 1) % SIDE].astype(bf16)


def total_body(own, g1, g2, g3, out):
    out[...] = (
        own[...] + g1[...].astype(f32) + g2[...].astype(f32) + g3[...].astype(f32)
    ).astype(bf16)


def layer(
    frames,
    span_source,
    adapter_weight,
    adapter_bias,
    norm_gain,
    qkv_weight,
    out_weight,
    k_cache,
    v_cache,
    lengths,
):
    rows = frames.shape[0]
    cols = adapter_weight.shape[1]
    meetings = lengths.shape[0]
    new = rows // meetings
    heads = 2 * SIDE
    ctx_rank = lax.axis_index("ctx")
    wt_rank = lax.axis_index("wt")
    place = jnp.stack(
        [wt_rank // 2, wt_rank % 2, ctx_rank // SIDE, ctx_rank % SIDE]
    ).astype(jnp.int32)

    positions = (lengths[:, None] + jnp.arange(new, dtype=jnp.int32)[None, :]).reshape(rows)
    half = HEAD // 2
    freq = 10000.0 ** (-2.0 * jnp.arange(half, dtype=f32) / HEAD)
    angle = positions.astype(f32)[:, None] * freq[None, :]
    cosine = jnp.cos(angle)
    sine = jnp.sin(angle)
    cosine = jnp.concatenate([cosine, cosine], axis=-1)
    sine = jnp.concatenate([-sine, sine], axis=-1)

    by_kind = jnp.transpose(qkv_weight, (1, 0, 2))
    feats = by_kind.shape[1]
    adapted, query_weight, other_weight = kernel_call(
        adapter_body,
        [
            (SMEM, span_source),
            (VMEM, frames),
            (VMEM, adapter_weight),
            (VMEM, adapter_bias.reshape(1, cols)),
            (ANY, by_kind),
        ],
        (near((rows, cols), bf16), near((feats, cols), bf16), near((2, feats, cols), bf16)),
        [pltpu.VMEM(frames.shape, bf16), pltpu.SemaphoreType.DMA((2,))],
    )
    column = stacked(from_ring(adapted, y_shift))
    stacks = from_ring(column, z_shift)

    query_weights = over_x(query_weight)
    other_weights = over_x(other_weight)
    swapped = swap_xy(out_weight)
    out_weights = over_x(swapped)

    gain = norm_gain.reshape(SIDE * SIDE, 1, cols)
    query, normed = kernel_call(
        query_body,
        [(SMEM, place)]
        + [(VMEM, s) for s in stacks]
        + [(VMEM, gain), (VMEM, cosine), (VMEM, sine)]
        + [(VMEM, w) for w in query_weights],
        (near((rows, cols), bf16), near((SIDE * SIDE, rows, cols), bf16)),
    )
    query_column = stacked(from_ring(query, y_shift))
    query_stacks = from_ring(query_column, z_shift)

    keys, values = kernel_call(
        key_value_body,
        [(SMEM, place), (VMEM, normed), (VMEM, cosine), (VMEM, sine)]
        + [(VMEM, w) for w in other_weights],
        (far((rows, cols), bf16), far((rows, cols), bf16)),
    )

    def history(step):
        return kernel_call(
            lambda *refs: history_body(step, *refs),
            [
                (SMEM, place),
                (SMEM, lengths),
                (VMEM, query_stacks[step]),
                (VMEM, k_cache),
                (VMEM, v_cache),
            ],
            near((heads * rows + 48, HEAD), bf16),
            [
                pltpu.VMEM((heads, rows, HEAD), f32),
                pltpu.VMEM((heads, rows, HEAD), bf16),
            ],
        )

    own = history(0)
    back = {j: z_shift(history(j), -j) for j in ORDER}
    block = near((2 * rows + 16, HEAD), bf16)
    mixed = kernel_call(
        row_mix_body,
        [(VMEM, p) for p in (own, back[1], back[2], back[3])],
        (block, block, block, block),
    )
    returned = {k: y_shift(mixed[k], -k) for k in ORDER}
    numer, new_stats = kernel_call(
        new_part_body,
        [(VMEM, query), (VMEM, keys), (VMEM, values)],
        (near((2 * rows, HEAD), f32), near((8, rows), f32)),
    )
    attended = kernel_call(
        final_mix_body,
        [(VMEM, p) for p in (mixed[0], returned[1], returned[2], returned[3], numer, new_stats)],
        near((rows, cols), bf16),
    )
    across = from_ring(attended, y_shift)
    part = near((rows, cols), bf16)
    sums = kernel_call(
        project_body,
        [(SMEM, place)] + [(VMEM, a) for a in across] + [(VMEM, w) for w in out_weights],
        (near((rows, cols), f32), part, part, part),
        [pltpu.VMEM((SIDE, rows, cols), bf16), pltpu.VMEM((SIDE, rows, cols), f32)],
    )
    got = [z_shift(sums[j], j) for j in ORDER]
    attn_out = kernel_call(
        total_body, [(VMEM, p) for p in (sums[0], *got)], far((rows, cols), bf16)
    )
    return attn_out, keys, values


def solution(mesh):
    return jax.shard_map(
        layer,
        mesh=mesh,
        in_specs=(
            P("wt", None),
            P("wt"),
            P(None, "ctx"),
            P("ctx"),
            P(),
            P("wt", None, "ctx"),
            P("ctx", "wt"),
            P("wt", "ctx", None),
            P("wt", "ctx", None),
            P("wt"),
        ),
        out_specs=(P("wt", "ctx"), P("wt", "ctx"), P("wt", "ctx")),
        check_vma=False,
    )
```

```python
import jax
import jax.numpy as jnp
from jax import lax
from jax.experimental import pallas as pl
from jax.experimental.pallas import tpu as pltpu
from jax.sharding import PartitionSpec as P


HEAD = 128
SIDE = 4
FLOOR = -1e30

bf16 = jnp.bfloat16
f32 = jnp.float32


def y_shift(x, k):
    pairs = [
        (y * SIDE + z, ((y + k) % SIDE) * SIDE + z) for y in range(SIDE) for z in range(SIDE)
    ]
    return lax.ppermute(x, "ctx", pairs)


def z_shift(x, k):
    pairs = [
        (y * SIDE + z, y * SIDE + (z + k) % SIDE) for y in range(SIDE) for z in range(SIDE)
    ]
    return lax.ppermute(x, "ctx", pairs)


def x_shift(x, k):
    pairs = [(2 * i + c, 2 * ((i + k) % SIDE) + c) for i in range(SIDE) for c in range(2)]
    return lax.ppermute(x, "wt", pairs)


def other_core(x):
    return lax.ppermute(x, "wt", [(i, i ^ 1) for i in range(2 * SIDE)])


def swap_xy(x):
    def place(i, y, z, c):
        return (y * SIDE + z) * 2 * SIDE + 2 * i + c

    pairs = [
        (place(i, y, z, c), place(y, i, z, c))
        for i in range(SIDE)
        for y in range(SIDE)
        for z in range(SIDE)
        for c in range(2)
    ]
    return lax.ppermute(x, ("ctx", "wt"), pairs)


ORDER = (1, 3, 2)


def from_ring(x, shift):
    got = {}
    for k in ORDER:
        got[k] = shift(x, k)
    return [x, got[1], got[2], got[3]]


def over_x(x):
    mine = from_ring(x, x_shift)
    return [p for m in mine for p in (m, other_core(m))]


VMEM = pl.BlockSpec(memory_space=pltpu.VMEM)
SMEM = pl.BlockSpec(memory_space=pltpu.SMEM)
ANY = pl.BlockSpec(memory_space=pl.ANY)
WHOLE = pl.BlockSpec()


def held(x):
    return pltpu.with_memory_space_constraint(x, pltpu.VMEM)


def outside(x):
    return pltpu.with_memory_space_constraint(x, pltpu.HBM)


def placed(spec, x):
    if spec is SMEM:
        return x
    return held(x) if spec is VMEM else outside(x)


def kernel_call(body, ins, out_shape, scratch=(), limit=12):
    single = not isinstance(out_shape, tuple)
    return pl.pallas_call(
        body,
        in_specs=[s for s, _ in ins],
        out_specs=VMEM if single else tuple(VMEM for _ in out_shape),
        out_shape=out_shape,
        scratch_shapes=list(scratch),
        compiler_params=pltpu.CompilerParams(vmem_limit_bytes=limit << 20),
    )(*[placed(s, a) for s, a in ins])


def near(dims, kind):
    return pltpu.VMEM(dims, kind)


def far(dims, kind):
    return jax.ShapeDtypeStruct(dims, kind)


def matmul(a, b):
    return jnp.dot(a, b, preferred_element_type=f32)


def matmul_t(a, b):
    return lax.dot_general(a, b, (((1,), (1,)), ((), ())), preferred_element_type=f32)


def adapter_body(source, frames, weight, bias, kinds, out, query_weight, other_weight, ordered, sems):
    copies = (
        pltpu.make_async_copy(kinds.at[0], query_weight, sems.at[0]),
        pltpu.make_async_copy(kinds.at[1:3], other_weight, sems.at[1]),
    )
    for copy in copies:
        copy.start()
    spans = source.shape[0]
    rows = frames.shape[0] // spans
    for g in range(spans):
        start = pl.multiple_of(source[g] * rows, rows)
        ordered[g * rows : (g + 1) * rows, :] = frames[pl.ds(start, rows), :]
    out[...] = (matmul(ordered[...], weight[...]) + bias[...]).astype(bf16)
    for copy in copies:
        copy.wait()


def stack_body(a0, a1, a2, a3, out):
    for k, a in enumerate((a0, a1, a2, a3)):
        out[k] = a[...]


def stacked(parts):
    dims = (SIDE, *parts[0].shape)
    return kernel_call(stack_body, [(VMEM, p) for p in parts], near(dims, bf16))


def spin(u, cosine, sine):
    return u * cosine + pltpu.roll(u, HEAD // 2, 1) * sine


def pieces_product(place, normed, weights, take):
    total = None
    for n, weight in enumerate(weights):
        shard = 2 * ((place[0] + SIDE - n // 2) % SIDE) + (place[1] + n) % 2
        w = take(weight)
        half = w.shape[0] // 2
        part = matmul(normed[2 * shard], w[:half]) + matmul(normed[2 * shard + 1], w[half:])
        total = part if total is None else total + part
    return total


def query_body(place, s0, s1, s2, s3, gain, cosine, sine, *rest):
    weights, (query, normed) = rest[:8], rest[8:]
    stacks = (s0, s1, s2, s3)
    rows = s0.shape[1]
    sums = jnp.zeros((rows, HEAD), f32)
    for stack in stacks:
        for k in range(SIDE):
            wide = stack[k].astype(f32)
            square = wide * wide
            sums = sums + (square[:, :HEAD] + square[:, HEAD:])
    width = SIDE * SIDE * s0.shape[2]
    factor = lax.rsqrt(jnp.sum(sums, axis=-1, keepdims=True) * (1.0 / width) + 1e-06)
    for j, stack in enumerate(stacks):
        for k in range(SIDE):
            block = SIDE * ((place[2] + SIDE - k) % SIDE) + (place[3] + SIDE - j) % SIDE
            normed[block] = (stack[k].astype(f32) * factor * gain[block]).astype(bf16)
    projected = pieces_product(place, normed, weights, lambda w: w[...])
    for h in range(projected.shape[1] // HEAD):
        cut = slice(h * HEAD, (h + 1) * HEAD)
        query[:, cut] = spin(projected[:, cut], cosine[...], sine[...]).astype(bf16)


def key_value_body(place, normed, cosine, sine, *rest):
    weights, (keys, values) = rest[:8], rest[8:]
    projected = pieces_product(place, normed, weights, lambda w: w[0])
    for h in range(projected.shape[1] // HEAD):
        cut = slice(h * HEAD, (h + 1) * HEAD)
        keys[:, cut] = spin(projected[:, cut], cosine[...], sine[...]).astype(bf16)
    values[...] = pieces_product(place, normed, weights, lambda w: w[1]).astype(bf16)


def split_in_three(x):
    high = x.astype(bf16).astype(f32)
    middle = (x - high).astype(bf16).astype(f32)
    return high, middle, x - high - middle


def soft_weights(scores, live):
    scores = jnp.where(live, scores, FLOOR)
    most = jnp.max(scores, axis=-1, keepdims=True)
    weights = jnp.where(live, jnp.exp(scores - most), 0.0)
    return weights, most, jnp.sum(weights, axis=-1, keepdims=True)


def history_body(step, place, lengths, stack, k_cache, v_cache, out, scores, weights):
    meetings, span = k_cache.shape[0], k_cache.shape[1]
    rows = stack.shape[1]
    new = rows // meetings
    heads = 2 * SIDE
    starts = []
    for k in range(SIDE):
        block = SIDE * ((place[2] + SIDE - k) % SIDE) + (place[3] + SIDE - step) % SIDE
        for h in range(2):
            starts.append(pl.multiple_of(block * 256 + h * HEAD, HEAD))
    for i, start in enumerate(starts):
        cut = slice(i % 2 * HEAD, (i % 2 + 1) * HEAD)
        for m in range(meetings):
            here = slice(m * new, (m + 1) * new)
            scores[i, here, :] = matmul_t(
                stack[i // 2, here, cut], k_cache[m, :, pl.ds(start, HEAD)]
            )
    first = (place[2] * SIDE + place[3]) * span
    spot = first + lax.broadcasted_iota(jnp.int32, (rows, span), 1)
    upper = lax.broadcasted_iota(jnp.int32, (rows, span), 0) < new
    live = spot < jnp.where(upper, lengths[0], lengths[1])
    lane = lax.broadcasted_iota(jnp.int32, (rows, HEAD), 1)
    stats = jnp.zeros((rows, HEAD), f32)
    for i in range(heads):
        weight, most, total = soft_weights(scores[i] * HEAD**-0.5, live)
        weights[i] = weight.astype(bf16)
        stats = jnp.where(lane == i, most, jnp.where(lane == heads + i, total, stats))
    for i, start in enumerate(starts):
        for m in range(meetings):
            here = slice(m * new, (m + 1) * new)
            at = i * rows + m * new
            out[at : at + new, :] = matmul(
                weights[i, here, :], v_cache[m, :, pl.ds(start, HEAD)]
            ).astype(bf16)
    turned = jnp.transpose(stats)[: 2 * heads]
    base = heads * rows
    for n, piece in enumerate(split_in_three(turned)):
        out[base + 16 * n : base + 16 * n + 16, :] = piece.astype(bf16)


def turned_columns(pieces, rows):
    used = sum(p.shape[0] for p in pieces)
    fill = [jnp.zeros((rows - used, pieces[0].shape[1]), f32)] if rows > used else []
    return jnp.transpose(jnp.concatenate(list(pieces) + fill, axis=0))


def row_mix_body(p0, p1, p2, p3, own, o1, o2, o3):
    parts = (p0, p1, p2, p3)
    outs = (own, o1, o2, o3)
    heads = 2 * SIDE
    rows = p0.shape[1]
    base = heads * rows
    tops, totals = [], []
    for p in parts:
        tail = p[base : base + 48, :].astype(f32)
        stats = tail[:16] + tail[16:32] + tail[32:]
        tops.append(stats[:heads])
        totals.append(stats[heads:])
    top = jnp.maximum(jnp.maximum(tops[0], tops[1]), jnp.maximum(tops[2], tops[3]))
    factors = [jnp.exp(t - top) for t in tops]
    total = sum(t * f for t, f in zip(totals, factors))
    columns = turned_columns(factors, rows)
    for h in range(heads):
        cut = slice(h * rows, (h + 1) * rows)
        mixed = None
        for i, p in enumerate(parts):
            at = i * heads + h
            term = p[cut, :].astype(f32) * columns[:, at : at + 1]
            mixed = term if mixed is None else mixed + term
        outs[h // 2][(h % 2) * rows : (h % 2 + 1) * rows, :] = mixed.astype(bf16)
    spread = [piece for pair in zip(split_in_three(top), split_in_three(total)) for piece in pair]
    for k in range(SIDE):
        cut = slice(2 * k, 2 * k + 2)
        outs[k][2 * rows : 2 * rows + 16, :] = jnp.concatenate(
            [piece[cut] for piece in spread] + [jnp.zeros((4, rows), f32)], axis=0
        ).astype(bf16)


def new_part_body(query, keys, values, numer, stats_out):
    rows = query.shape[0]
    new = rows // 2
    causal = lax.broadcasted_iota(jnp.int32, (new, new), 0) >= lax.broadcasted_iota(
        jnp.int32, (new, new), 1
    )
    lane = lax.broadcasted_iota(jnp.int32, (new, HEAD), 1)
    stats = []
    for m in range(2):
        here = slice(m * new, (m + 1) * new)
        tile = jnp.zeros((new, HEAD), f32)
        for h in range(2):
            cut = slice(h * HEAD, (h + 1) * HEAD)
            weight, most, total = soft_weights(
                matmul_t(query[here, cut], keys[here, cut]) * HEAD**-0.5, causal
            )
            numer[h * rows + m * new : h * rows + (m + 1) * new, :] = matmul(
                weight.astype(bf16), values[here, cut]
            )
            tile = jnp.where(lane == h, most, jnp.where(lane == 2 + h, total, tile))
        stats.append(tile)
    stats_out[...] = jnp.transpose(jnp.concatenate(stats, axis=0))[:8]


def final_mix_body(p0, p1, p2, p3, numer, new_stats, out):
    parts = (p0, p1, p2, p3)
    rows = numer.shape[0] // 2
    tops, totals = [], []
    for p in parts:
        tail = p[2 * rows : 2 * rows + 16, :].astype(f32)
        tops.append(tail[0:2] + tail[4:6] + tail[8:10])
        totals.append(tail[2:4] + tail[6:8] + tail[10:12])
    tops.append(new_stats[0:2])
    totals.append(new_stats[2:4])
    top = tops[0]
    for t in tops[1:]:
        top = jnp.maximum(top, t)
    factors = [jnp.exp(t - top) for t in tops]
    total = sum(t * f for t, f in zip(totals, factors))
    columns = turned_columns([f / total for f in factors], rows)
    for h in range(2):
        cut = slice(h * rows, (h + 1) * rows)
        mixed = numer[cut, :] * columns[:, 8 + h : 9 + h]
        for i, p in enumerate(parts):
            mixed = mixed + p[cut, :].astype(f32) * columns[:, 2 * i + h : 2 * i + h + 1]
        out[:, h * HEAD : (h + 1) * HEAD] = mixed.astype(bf16)


def project_body(place, a0, a1, a2, a3, *rest):
    weights, (own, o1, o2, o3, across, sums) = rest[:8], rest[8:]
    for k, a in enumerate((a0, a1, a2, a3)):
        across[(place[2] + SIDE - k) % SIDE] = a[...]
    for c in range(2):
        total = None
        for j in range(SIDE):
            part = matmul(across[(place[0] + SIDE - j) % SIDE], weights[2 * j + c][...])
            total = part if total is None else total + part
        first = 2 * ((place[1] + c) % 2)
        sums[first] = total[:, :256]
        sums[first + 1] = total[:, 256:]
    own[...] = sums[place[3]]
    for j, o in enumerate((o1, o2, o3)):
        o[...] = sums[(place[3] + j + 1) % SIDE].astype(bf16)


def total_body(own, g1, g2, g3, out):
    out[...] = (
        own[...] + g1[...].astype(f32) + g2[...].astype(f32) + g3[...].astype(f32)
    ).astype(bf16)


def layer(
    frames,
    span_source,
    adapter_weight,
    adapter_bias,
    norm_gain,
    qkv_weight,
    out_weight,
    k_cache,
    v_cache,
    lengths,
):
    rows = frames.shape[0]
    cols = adapter_weight.shape[1]
    meetings = lengths.shape[0]
    new = rows // meetings
    heads = 2 * SIDE
    ctx_rank = lax.axis_index("ctx")
    wt_rank = lax.axis_index("wt")
    place = jnp.stack(
        [wt_rank // 2, wt_rank % 2, ctx_rank // SIDE, ctx_rank % SIDE]
    ).astype(jnp.int32)

    token = lax.broadcasted_iota(jnp.int32, (rows, HEAD), 0)
    lane = lax.broadcasted_iota(jnp.int32, (rows, HEAD), 1)
    half = HEAD // 2
    positions = jnp.where(token < new, lengths[0], lengths[1] - new) + token
    freq = 10000.0 ** (-2.0 * (jnp.arange(HEAD, dtype=jnp.int32) % half).astype(f32) / HEAD)
    angle = positions.astype(f32) * freq[None, :]
    cosine = jnp.cos(angle)
    sine = jnp.where(lane < half, -jnp.sin(angle), jnp.sin(angle))

    by_kind = jnp.transpose(qkv_weight, (1, 0, 2))
    feats = by_kind.shape[1]
    adapted, query_weight, other_weight = kernel_call(
        adapter_body,
        [
            (SMEM, span_source),
            (WHOLE, frames),
            (WHOLE, adapter_weight),
            (WHOLE, adapter_bias.reshape(1, cols)),
            (ANY, by_kind),
        ],
        (near((rows, cols), bf16), near((feats, cols), bf16), near((2, feats, cols), bf16)),
        [pltpu.VMEM(frames.shape, bf16), pltpu.SemaphoreType.DMA((2,))],
    )
    column = stacked(from_ring(adapted, y_shift))
    stacks = from_ring(column, z_shift)

    query_weights = over_x(query_weight)
    other_weights = over_x(other_weight)
    swapped = swap_xy(out_weight)
    out_weights = over_x(swapped)

    gain = norm_gain.reshape(SIDE * SIDE, 1, cols)
    query, normed = kernel_call(
        query_body,
        [(SMEM, place)]
        + [(VMEM, s) for s in stacks]
        + [(VMEM, gain), (VMEM, cosine), (VMEM, sine)]
        + [(VMEM, w) for w in query_weights],
        (near((rows, cols), bf16), near((SIDE * SIDE, rows, cols), bf16)),
    )
    query_column = stacked(from_ring(query, y_shift))
    query_stacks = from_ring(query_column, z_shift)

    keys, values = kernel_call(
        key_value_body,
        [(SMEM, place), (VMEM, normed), (VMEM, cosine), (VMEM, sine)]
        + [(VMEM, w) for w in other_weights],
        (near((rows, cols), bf16), near((rows, cols), bf16)),
    )

    def history(step):
        return kernel_call(
            lambda *refs: history_body(step, *refs),
            [
                (SMEM, place),
                (SMEM, lengths),
                (VMEM, query_stacks[step]),
                (VMEM, k_cache),
                (VMEM, v_cache),
            ],
            near((heads * rows + 48, HEAD), bf16),
            [
                pltpu.VMEM((heads, rows, HEAD), f32),
                pltpu.VMEM((heads, rows, HEAD), bf16),
            ],
        )

    own = history(0)
    back = {j: z_shift(history(j), -j) for j in ORDER}
    block = near((2 * rows + 16, HEAD), bf16)
    mixed = kernel_call(
        row_mix_body,
        [(VMEM, p) for p in (own, back[1], back[2], back[3])],
        (block, block, block, block),
    )
    returned = {k: y_shift(mixed[k], -k) for k in ORDER}
    numer, new_stats = kernel_call(
        new_part_body,
        [(VMEM, query), (VMEM, keys), (VMEM, values)],
        (near((2 * rows, HEAD), f32), near((8, rows), f32)),
    )
    attended = kernel_call(
        final_mix_body,
        [(VMEM, p) for p in (mixed[0], returned[1], returned[2], returned[3], numer, new_stats)],
        near((rows, cols), bf16),
    )
    across = from_ring(attended, y_shift)
    part = near((rows, cols), bf16)
    sums = kernel_call(
        project_body,
        [(SMEM, place)] + [(VMEM, a) for a in across] + [(VMEM, w) for w in out_weights],
        (near((rows, cols), f32), part, part, part),
        [pltpu.VMEM((SIDE, rows, cols), bf16), pltpu.VMEM((SIDE, rows, cols), f32)],
    )
    got = [z_shift(sums[j], j) for j in ORDER]
    attn_out = kernel_call(
        total_body, [(VMEM, p) for p in (sums[0], *got)], far((rows, cols), bf16)
    )
    return attn_out, keys, values


def solution(mesh):
    return jax.shard_map(
        layer,
        mesh=mesh,
        in_specs=(
            P("wt", None),
            P("wt"),
            P(None, "ctx"),
            P("ctx"),
            P(),
            P("wt", None, "ctx"),
            P("ctx", "wt"),
            P("wt", "ctx", None),
            P("wt", "ctx", None),
            P("wt"),
        ),
        out_specs=(P("wt", "ctx"), P("wt", "ctx"), P("wt", "ctx")),
        check_vma=False,
    )
```

```python
import jax
import jax.numpy as jnp
import numpy as np
from jax import lax
from jax.experimental import pallas as pl
from jax.experimental.pallas import tpu as pltpu
from jax.sharding import PartitionSpec as P


HEAD = 128
SIDE = 4
FLOOR = -1e30

bf16 = jnp.bfloat16
f32 = jnp.float32


def y_shift(x, k):
    pairs = [
        (y * SIDE + z, ((y + k) % SIDE) * SIDE + z) for y in range(SIDE) for z in range(SIDE)
    ]
    return lax.ppermute(x, "ctx", pairs)


def z_shift(x, k):
    pairs = [
        (y * SIDE + z, y * SIDE + (z + k) % SIDE) for y in range(SIDE) for z in range(SIDE)
    ]
    return lax.ppermute(x, "ctx", pairs)


def x_shift(x, k):
    pairs = [(2 * i + c, 2 * ((i + k) % SIDE) + c) for i in range(SIDE) for c in range(2)]
    return lax.ppermute(x, "wt", pairs)


def other_core(x):
    return lax.ppermute(x, "wt", [(i, i ^ 1) for i in range(2 * SIDE)])


def swap_xy(x):
    def place(i, y, z, c):
        return (y * SIDE + z) * 2 * SIDE + 2 * i + c

    pairs = [
        (place(i, y, z, c), place(y, i, z, c))
        for i in range(SIDE)
        for y in range(SIDE)
        for z in range(SIDE)
        for c in range(2)
    ]
    return lax.ppermute(x, ("ctx", "wt"), pairs)


ORDER = (1, 3, 2)


def from_ring(x, shift):
    got = {}
    for k in ORDER:
        got[k] = shift(x, k)
    return [x, got[1], got[2], got[3]]


def over_x(x):
    mine = from_ring(x, x_shift)
    both = []
    for m in mine:
        both += [m, other_core(m)]
    return both


VMEM = pl.BlockSpec(memory_space=pltpu.VMEM)
SMEM = pl.BlockSpec(memory_space=pltpu.SMEM)
ANY = pl.BlockSpec(memory_space=pl.ANY)
WHOLE = pl.BlockSpec()


def held(x):
    return pltpu.with_memory_space_constraint(x, pltpu.VMEM)


def outside(x):
    return pltpu.with_memory_space_constraint(x, pltpu.HBM)


def placed(spec, x):
    return held(x) if spec is VMEM else outside(x)


def kernel_call(body, ins, out_shape, scratch=(), limit=12):
    single = not isinstance(out_shape, tuple)
    return pl.pallas_call(
        body,
        in_specs=[s for s, _ in ins],
        out_specs=VMEM if single else tuple(VMEM for _ in out_shape),
        out_shape=out_shape,
        scratch_shapes=list(scratch),
        compiler_params=pltpu.CompilerParams(vmem_limit_bytes=limit << 20),
    )(*[placed(s, a) for s, a in ins])


def near(dims, kind):
    return pltpu.VMEM(dims, kind)


def far(dims, kind):
    return jax.ShapeDtypeStruct(dims, kind)


def position():
    ctx_rank = lax.axis_index("ctx")
    wt_rank = lax.axis_index("wt")
    return wt_rank // 2, wt_rank % 2, ctx_rank // SIDE, ctx_rank % SIDE


def matmul(a, b):
    return jnp.dot(a, b, preferred_element_type=f32)


def matmul_t(a, b):
    return lax.dot_general(a, b, (((1,), (1,)), ((), ())), preferred_element_type=f32)


def turns(count, step):
    freq = 10000.0 ** (-2.0 * (np.arange(HEAD) % (HEAD // 2)) / HEAD)
    angle = step * np.arange(count)[:, None] * freq[None, :]
    return np.stack([np.cos(angle), np.sin(angle)]).astype(np.float32)


def rope_tables(lengths, coarse, fine, cosine, sine, new):
    lane = lax.broadcasted_iota(jnp.int32, (new, HEAD), 1)
    for m in range(cosine.shape[0] // new):
        high = lengths[m] // new
        low = lengths[m] - high * new
        c1, s1 = coarse[0, pl.ds(high, 1), :], coarse[1, pl.ds(high, 1), :]
        c2, s2 = fine[0, pl.ds(low, new), :], fine[1, pl.ds(low, new), :]
        here = slice(m * new, (m + 1) * new)
        cosine[here, :] = c1 * c2 - s1 * s2
        value = s1 * c2 + c1 * s2
        sine[here, :] = jnp.where(lane < HEAD // 2, -value, value)


def adapter_body(
    source,
    lengths,
    frames,
    weight,
    bias,
    coarse,
    fine,
    kinds,
    out,
    query_weight,
    other_weight,
    cosine,
    sine,
    ordered,
    sems,
):
    copies = (
        pltpu.make_async_copy(kinds.at[0], query_weight, sems.at[0]),
        pltpu.make_async_copy(kinds.at[1:3], other_weight, sems.at[1]),
    )
    for copy in copies:
        copy.start()
    rope_tables(lengths, coarse, fine, cosine, sine, fine.shape[1] // 2)
    spans = source.shape[0]
    rows = frames.shape[0] // spans
    for g in range(spans):
        start = pl.multiple_of(source[g] * rows, rows)
        ordered[g * rows : (g + 1) * rows, :] = frames[pl.ds(start, rows), :]
    out[...] = (matmul(ordered[...], weight[...]) + bias[...]).astype(bf16)
    for copy in copies:
        copy.wait()


def stack_body(a0, a1, a2, a3, out):
    for k, a in enumerate((a0, a1, a2, a3)):
        out[k] = a[...]


def stacked(parts):
    dims = (SIDE, *parts[0].shape)
    return kernel_call(stack_body, [(VMEM, p) for p in parts], near(dims, bf16))


def spin(u, cosine, sine):
    return u * cosine + pltpu.roll(u, HEAD // 2, 1) * sine


def pieces_product(place, normed, weights, take):
    total = None
    for n, weight in enumerate(weights):
        shard = 2 * ((place[0] + SIDE - n // 2) % SIDE) + (place[1] + n) % 2
        w = take(weight)
        half = w.shape[0] // 2
        part = matmul(normed[2 * shard], w[:half]) + matmul(normed[2 * shard + 1], w[half:])
        total = part if total is None else total + part
    return total


def query_body(s0, s1, s2, s3, gain, cosine, sine, *rest):
    weights, (query, normed) = rest[:8], rest[8:]
    place = position()
    stacks = (s0, s1, s2, s3)
    rows = s0.shape[1]
    sums = jnp.zeros((rows, HEAD), f32)
    for stack in stacks:
        for k in range(SIDE):
            wide = stack[k].astype(f32)
            square = wide * wide
            sums = sums + (square[:, :HEAD] + square[:, HEAD:])
    width = SIDE * SIDE * s0.shape[2]
    factor = lax.rsqrt(jnp.sum(sums, axis=-1, keepdims=True) * (1.0 / width) + 1e-06)
    for j, stack in enumerate(stacks):
        for k in range(SIDE):
            block = SIDE * ((place[2] + SIDE - k) % SIDE) + (place[3] + SIDE - j) % SIDE
            normed[block] = (stack[k].astype(f32) * factor * gain[block]).astype(bf16)
    projected = pieces_product(place, normed, weights, lambda w: w[...])
    for h in range(projected.shape[1] // HEAD):
        cut = slice(h * HEAD, (h + 1) * HEAD)
        query[:, cut] = spin(projected[:, cut], cosine[...], sine[...]).astype(bf16)


def key_value_body(normed, cosine, sine, *rest):
    weights, (keys, values) = rest[:8], rest[8:]
    place = position()
    projected = pieces_product(place, normed, weights, lambda w: w[0])
    for h in range(projected.shape[1] // HEAD):
        cut = slice(h * HEAD, (h + 1) * HEAD)
        keys[:, cut] = spin(projected[:, cut], cosine[...], sine[...]).astype(bf16)
    values[...] = pieces_product(place, normed, weights, lambda w: w[1]).astype(bf16)


def split_in_three(x):
    high = x.astype(bf16).astype(f32)
    middle = (x - high).astype(bf16).astype(f32)
    return high, middle, x - high - middle


def soft_weights(scores, live):
    scores = jnp.where(live, scores, FLOOR)
    most = jnp.max(scores, axis=-1, keepdims=True)
    weights = jnp.where(live, jnp.exp(scores - most), 0.0)
    return weights, most, jnp.sum(weights, axis=-1, keepdims=True)


def history_body(step, lengths, stack, k_cache, v_cache, out, scores, weights):
    meetings, span = k_cache.shape[0], k_cache.shape[1]
    place = position()
    rows = stack.shape[1]
    new = rows // meetings
    heads = 2 * SIDE
    starts = []
    for k in range(SIDE):
        block = SIDE * ((place[2] + SIDE - k) % SIDE) + (place[3] + SIDE - step) % SIDE
        for h in range(2):
            starts.append(pl.multiple_of(block * 256 + h * HEAD, HEAD))
    for i, start in enumerate(starts):
        cut = slice(i % 2 * HEAD, (i % 2 + 1) * HEAD)
        for m in range(meetings):
            here = slice(m * new, (m + 1) * new)
            scores[i, here, :] = matmul_t(
                stack[i // 2, here, cut], k_cache[m, :, pl.ds(start, HEAD)]
            )
    first = (place[2] * SIDE + place[3]) * span
    spot = first + lax.broadcasted_iota(jnp.int32, (rows, span), 1)
    upper = lax.broadcasted_iota(jnp.int32, (rows, span), 0) < new
    live = spot < jnp.where(upper, lengths[0], lengths[1])
    lane = lax.broadcasted_iota(jnp.int32, (rows, HEAD), 1)
    stats = jnp.zeros((rows, HEAD), f32)
    for i in range(heads):
        weight, most, total = soft_weights(scores[i] * HEAD**-0.5, live)
        weights[i] = weight.astype(bf16)
        stats = jnp.where(lane == i, most, jnp.where(lane == heads + i, total, stats))
    for i, start in enumerate(starts):
        for m in range(meetings):
            here = slice(m * new, (m + 1) * new)
            at = i * rows + m * new
            out[at : at + new, :] = matmul(
                weights[i, here, :], v_cache[m, :, pl.ds(start, HEAD)]
            ).astype(bf16)
    turned = jnp.transpose(stats)[: 2 * heads]
    base = heads * rows
    for n, piece in enumerate(split_in_three(turned)):
        out[base + 16 * n : base + 16 * n + 16, :] = piece.astype(bf16)


def turned_columns(pieces, rows):
    used = sum(p.shape[0] for p in pieces)
    fill = [jnp.zeros((rows - used, pieces[0].shape[1]), f32)] if rows > used else []
    return jnp.transpose(jnp.concatenate(list(pieces) + fill, axis=0))


def row_mix_body(p0, p1, p2, p3, own, o1, o2, o3):
    parts = (p0, p1, p2, p3)
    outs = (own, o1, o2, o3)
    heads = 2 * SIDE
    rows = p0.shape[1]
    base = heads * rows
    tops, totals = [], []
    for p in parts:
        tail = p[base : base + 48, :].astype(f32)
        stats = tail[:16] + tail[16:32] + tail[32:]
        tops.append(stats[:heads])
        totals.append(stats[heads:])
    top = jnp.maximum(jnp.maximum(tops[0], tops[1]), jnp.maximum(tops[2], tops[3]))
    factors = [jnp.exp(t - top) for t in tops]
    total = sum(t * f for t, f in zip(totals, factors))
    columns = turned_columns(factors, rows)
    for h in range(heads):
        cut = slice(h * rows, (h + 1) * rows)
        mixed = None
        for i, p in enumerate(parts):
            at = i * heads + h
            term = p[cut, :].astype(f32) * columns[:, at : at + 1]
            mixed = term if mixed is None else mixed + term
        outs[h // 2][(h % 2) * rows : (h % 2 + 1) * rows, :] = mixed.astype(bf16)
    spread = [piece for pair in zip(split_in_three(top), split_in_three(total)) for piece in pair]
    for k in range(SIDE):
        cut = slice(2 * k, 2 * k + 2)
        outs[k][2 * rows : 2 * rows + 16, :] = jnp.concatenate(
            [piece[cut] for piece in spread] + [jnp.zeros((4, rows), f32)], axis=0
        ).astype(bf16)


def new_part_body(query, keys, values, numer, stats_out):
    rows = query.shape[0]
    new = rows // 2
    causal = lax.broadcasted_iota(jnp.int32, (new, new), 0) >= lax.broadcasted_iota(
        jnp.int32, (new, new), 1
    )
    lane = lax.broadcasted_iota(jnp.int32, (new, HEAD), 1)
    stats = []
    for m in range(2):
        here = slice(m * new, (m + 1) * new)
        tile = jnp.zeros((new, HEAD), f32)
        for h in range(2):
            cut = slice(h * HEAD, (h + 1) * HEAD)
            weight, most, total = soft_weights(
                matmul_t(query[here, cut], keys[here, cut]) * HEAD**-0.5, causal
            )
            numer[h * rows + m * new : h * rows + (m + 1) * new, :] = matmul(
                weight.astype(bf16), values[here, cut]
            )
            tile = jnp.where(lane == h, most, jnp.where(lane == 2 + h, total, tile))
        stats.append(tile)
    stats_out[...] = jnp.transpose(jnp.concatenate(stats, axis=0))[:8]


def final_mix_body(p0, p1, p2, p3, numer, new_stats, out):
    parts = (p0, p1, p2, p3)
    rows = numer.shape[0] // 2
    tops, totals = [], []
    for p in parts:
        tail = p[2 * rows : 2 * rows + 16, :].astype(f32)
        tops.append(tail[0:2] + tail[4:6] + tail[8:10])
        totals.append(tail[2:4] + tail[6:8] + tail[10:12])
    tops.append(new_stats[0:2])
    totals.append(new_stats[2:4])
    top = tops[0]
    for t in tops[1:]:
        top = jnp.maximum(top, t)
    factors = [jnp.exp(t - top) for t in tops]
    total = sum(t * f for t, f in zip(totals, factors))
    columns = turned_columns([f / total for f in factors], rows)
    for h in range(2):
        cut = slice(h * rows, (h + 1) * rows)
        mixed = numer[cut, :] * columns[:, 8 + h : 9 + h]
        for i, p in enumerate(parts):
            mixed = mixed + p[cut, :].astype(f32) * columns[:, 2 * i + h : 2 * i + h + 1]
        out[:, h * HEAD : (h + 1) * HEAD] = mixed.astype(bf16)


def project_body(a0, a1, a2, a3, *rest):
    weights, (own, o1, o2, o3, across, sums) = rest[:8], rest[8:]
    place = position()
    for k, a in enumerate((a0, a1, a2, a3)):
        across[(place[2] + SIDE - k) % SIDE] = a[...]
    for c in range(2):
        total = None
        for j in range(SIDE):
            part = matmul(across[(place[0] + SIDE - j) % SIDE], weights[2 * j + c][...])
            total = part if total is None else total + part
        first = 2 * ((place[1] + c) % 2)
        sums[first] = total[:, :256]
        sums[first + 1] = total[:, 256:]
    own[...] = sums[place[3]]
    for j, o in enumerate((o1, o2, o3)):
        o[...] = sums[(place[3] + j + 1) % SIDE].astype(bf16)


def total_body(own, g1, g2, g3, out):
    out[...] = (
        own[...] + g1[...].astype(f32) + g2[...].astype(f32) + g3[...].astype(f32)
    ).astype(bf16)


def layer(
    frames,
    span_source,
    adapter_weight,
    adapter_bias,
    norm_gain,
    qkv_weight,
    out_weight,
    k_cache,
    v_cache,
    lengths,
):
    rows = frames.shape[0]
    cols = adapter_weight.shape[1]
    meetings = lengths.shape[0]
    new = rows // meetings
    heads = 2 * SIDE
    by_kind = jnp.transpose(qkv_weight, (1, 0, 2))
    feats = by_kind.shape[1]
    longest = SIDE * SIDE * k_cache.shape[1]
    coarse = jnp.asarray(turns(longest // new + 8, new))
    fine = jnp.asarray(turns(2 * new, 1))
    adapted, query_weight, other_weight, cosine, sine = kernel_call(
        adapter_body,
        [
            (SMEM, span_source),
            (SMEM, lengths),
            (WHOLE, frames),
            (WHOLE, adapter_weight),
            (WHOLE, adapter_bias.reshape(1, cols)),
            (WHOLE, coarse),
            (WHOLE, fine),
            (ANY, by_kind),
        ],
        (
            near((rows, cols), bf16),
            near((feats, cols), bf16),
            near((2, feats, cols), bf16),
            near((rows, HEAD), f32),
            near((rows, HEAD), f32),
        ),
        [pltpu.VMEM(frames.shape, bf16), pltpu.SemaphoreType.DMA((2,))],
    )
    column = stacked(from_ring(adapted, y_shift))
    stacks = from_ring(column, z_shift)

    query_weights = over_x(query_weight)
    other_weights = over_x(other_weight)
    swapped = swap_xy(out_weight)
    out_weights = over_x(swapped)

    gain = norm_gain.reshape(SIDE * SIDE, 1, cols)
    query, normed = kernel_call(
        query_body,
        [(VMEM, s) for s in stacks]
        + [(VMEM, gain), (VMEM, cosine), (VMEM, sine)]
        + [(VMEM, w) for w in query_weights],
        (
            near((rows, cols), bf16),
            near((SIDE * SIDE, rows, cols), bf16),
        ),
    )
    query_column = stacked(from_ring(query, y_shift))
    query_stacks = from_ring(query_column, z_shift)

    keys, values = kernel_call(
        key_value_body,
        [(VMEM, normed), (VMEM, cosine), (VMEM, sine)]
        + [(VMEM, w) for w in other_weights],
        (near((rows, cols), bf16), near((rows, cols), bf16)),
    )

    def history(step):
        return kernel_call(
            lambda *refs: history_body(step, *refs),
            [
                (SMEM, lengths),
                (VMEM, query_stacks[step]),
                (VMEM, k_cache),
                (VMEM, v_cache),
            ],
            near((heads * rows + 48, HEAD), bf16),
            [
                pltpu.VMEM((heads, rows, HEAD), f32),
                pltpu.VMEM((heads, rows, HEAD), bf16),
            ],
        )

    own = history(0)
    back = {j: z_shift(history(j), -j) for j in ORDER}
    block = near((2 * rows + 16, HEAD), bf16)
    mixed = kernel_call(
        row_mix_body,
        [(VMEM, p) for p in (own, back[1], back[2], back[3])],
        (block, block, block, block),
    )
    returned = {k: y_shift(mixed[k], -k) for k in ORDER}
    numer, new_stats = kernel_call(
        new_part_body,
        [(VMEM, query), (VMEM, keys), (VMEM, values)],
        (near((2 * rows, HEAD), f32), near((8, rows), f32)),
    )
    attended = kernel_call(
        final_mix_body,
        [(VMEM, p) for p in (mixed[0], returned[1], returned[2], returned[3], numer, new_stats)],
        near((rows, cols), bf16),
    )
    across = from_ring(attended, y_shift)
    part = near((rows, cols), bf16)
    sums = kernel_call(
        project_body,
        [(VMEM, a) for a in across] + [(VMEM, w) for w in out_weights],
        (near((rows, cols), f32), part, part, part),
        [pltpu.VMEM((SIDE, rows, cols), bf16), pltpu.VMEM((SIDE, rows, cols), f32)],
    )
    got = [z_shift(sums[j], j) for j in ORDER]
    attn_out = kernel_call(
        total_body, [(VMEM, p) for p in (sums[0], *got)], far((rows, cols), bf16)
    )
    return attn_out, keys, values


def solution(mesh):
    return jax.shard_map(
        layer,
        mesh=mesh,
        in_specs=(
            P("wt", None),
            P("wt"),
            P(None, "ctx"),
            P("ctx"),
            P(),
            P("wt", None, "ctx"),
            P("ctx", "wt"),
            P("wt", "ctx", None),
            P("wt", "ctx", None),
            P("wt"),
        ),
        out_specs=(P("wt", "ctx"), P("wt", "ctx"), P("wt", "ctx")),
        check_vma=False,
    )
```

```python
import jax
import jax.numpy as jnp
import numpy as np
from jax import lax
from jax.experimental import pallas as pl
from jax.experimental.pallas import tpu as pltpu
from jax.sharding import PartitionSpec as P


HEAD = 128
SIDE = 4
FLOOR = -1e30

bf16 = jnp.bfloat16
f32 = jnp.float32


def y_shift(x, k):
    pairs = [
        (y * SIDE + z, ((y + k) % SIDE) * SIDE + z) for y in range(SIDE) for z in range(SIDE)
    ]
    return lax.ppermute(x, "ctx", pairs)


def z_shift(x, k):
    pairs = [
        (y * SIDE + z, y * SIDE + (z + k) % SIDE) for y in range(SIDE) for z in range(SIDE)
    ]
    return lax.ppermute(x, "ctx", pairs)


def x_shift(x, k):
    pairs = [(2 * i + c, 2 * ((i + k) % SIDE) + c) for i in range(SIDE) for c in range(2)]
    return lax.ppermute(x, "wt", pairs)


def other_core(x):
    return lax.ppermute(x, "wt", [(i, i ^ 1) for i in range(2 * SIDE)])


def swap_xy(x):
    def place(i, y, z, c):
        return (y * SIDE + z) * 2 * SIDE + 2 * i + c

    pairs = [
        (place(i, y, z, c), place(y, i, z, c))
        for i in range(SIDE)
        for y in range(SIDE)
        for z in range(SIDE)
        for c in range(2)
    ]
    return lax.ppermute(x, ("ctx", "wt"), pairs)


ORDER = (1, 3, 2)


def from_ring(x, shift):
    got = {}
    for k in ORDER:
        got[k] = shift(x, k)
    return [x, got[1], got[2], got[3]]


def over_x(x):
    mine = from_ring(x, x_shift)
    both = []
    for m in mine:
        both += [m, other_core(m)]
    return both


VMEM = pl.BlockSpec(memory_space=pltpu.VMEM)
SMEM = pl.BlockSpec(memory_space=pltpu.SMEM)
ANY = pl.BlockSpec(memory_space=pl.ANY)
WHOLE = pl.BlockSpec()


def held(x):
    return pltpu.with_memory_space_constraint(x, pltpu.VMEM)


def outside(x):
    return pltpu.with_memory_space_constraint(x, pltpu.HBM)


def placed(spec, x):
    return held(x) if spec is VMEM else outside(x)


def kernel_call(body, ins, out_shape, scratch=(), limit=12):
    single = not isinstance(out_shape, tuple)
    return pl.pallas_call(
        body,
        in_specs=[s for s, _ in ins],
        out_specs=VMEM if single else tuple(VMEM for _ in out_shape),
        out_shape=out_shape,
        scratch_shapes=list(scratch),
        compiler_params=pltpu.CompilerParams(vmem_limit_bytes=limit << 20),
    )(*[placed(s, a) for s, a in ins])


def near(dims, kind):
    return pltpu.VMEM(dims, kind)


def far(dims, kind):
    return jax.ShapeDtypeStruct(dims, kind)


def position():
    ctx_rank = lax.axis_index("ctx")
    wt_rank = lax.axis_index("wt")
    return wt_rank // 2, wt_rank % 2, ctx_rank // SIDE, ctx_rank % SIDE


def matmul(a, b):
    return jnp.dot(a, b, preferred_element_type=f32)


def matmul_t(a, b):
    return lax.dot_general(a, b, (((1,), (1,)), ((), ())), preferred_element_type=f32)


def turns(count, step):
    freq = 10000.0 ** (-2.0 * (np.arange(HEAD) % (HEAD // 2)) / HEAD)
    angle = step * np.arange(count)[:, None] * freq[None, :]
    return np.stack([np.cos(angle), np.sin(angle)]).astype(np.float32)


def rope_tables(lengths, coarse, fine, cosine, sine, new):
    lane = lax.broadcasted_iota(jnp.int32, (new, HEAD), 1)
    for m in range(cosine.shape[0] // new):
        high = lengths[m] // new
        low = lengths[m] - high * new
        c1, s1 = coarse[0, pl.ds(high, 1), :], coarse[1, pl.ds(high, 1), :]
        c2, s2 = fine[0, pl.ds(low, new), :], fine[1, pl.ds(low, new), :]
        here = slice(m * new, (m + 1) * new)
        cosine[here, :] = c1 * c2 - s1 * s2
        value = s1 * c2 + c1 * s2
        sine[here, :] = jnp.where(lane < HEAD // 2, -value, value)


def adapter_body(
    source,
    lengths,
    frames,
    weight,
    bias,
    coarse,
    fine,
    kinds,
    out,
    query_weight,
    other_weight,
    cosine,
    sine,
    ordered,
    sems,
):
    copies = (
        pltpu.make_async_copy(kinds.at[0], query_weight, sems.at[0]),
        pltpu.make_async_copy(kinds.at[1:3], other_weight, sems.at[1]),
    )
    for copy in copies:
        copy.start()
    rope_tables(lengths, coarse, fine, cosine, sine, fine.shape[1] // 2)
    spans = source.shape[0]
    rows = frames.shape[0] // spans
    for g in range(spans):
        start = pl.multiple_of(source[g] * rows, rows)
        ordered[g * rows : (g + 1) * rows, :] = frames[pl.ds(start, rows), :]
    out[...] = (matmul(ordered[...], weight[...]) + bias[...]).astype(bf16)
    for copy in copies:
        copy.wait()


def stack_body(a0, a1, a2, a3, out):
    for k, a in enumerate((a0, a1, a2, a3)):
        out[k] = a[...]


def stacked(parts):
    dims = (SIDE, *parts[0].shape)
    return kernel_call(stack_body, [(VMEM, p) for p in parts], near(dims, bf16))


def spin(u, cosine, sine):
    return u * cosine + pltpu.roll(u, HEAD // 2, 1) * sine


def pieces_product(place, normed, weights, take):
    total = None
    for n, weight in enumerate(weights):
        shard = 2 * ((place[0] + SIDE - n // 2) % SIDE) + (place[1] + n) % 2
        w = take(weight)
        half = w.shape[0] // 2
        part = matmul(normed[2 * shard], w[:half]) + matmul(normed[2 * shard + 1], w[half:])
        total = part if total is None else total + part
    return total


def query_body(s0, s1, s2, s3, gain, cosine, sine, *rest):
    weights, (query, normed) = rest[:8], rest[8:]
    place = position()
    stacks = (s0, s1, s2, s3)
    rows = s0.shape[1]
    sums = jnp.zeros((rows, HEAD), f32)
    for stack in stacks:
        for k in range(SIDE):
            wide = stack[k].astype(f32)
            square = wide * wide
            sums = sums + (square[:, :HEAD] + square[:, HEAD:])
    width = SIDE * SIDE * s0.shape[2]
    factor = lax.rsqrt(jnp.sum(sums, axis=-1, keepdims=True) * (1.0 / width) + 1e-06)
    for j, stack in enumerate(stacks):
        for k in range(SIDE):
            block = SIDE * ((place[2] + SIDE - k) % SIDE) + (place[3] + SIDE - j) % SIDE
            normed[block] = (stack[k].astype(f32) * factor * gain[block]).astype(bf16)
    projected = pieces_product(place, normed, weights, lambda w: w[...])
    for h in range(projected.shape[1] // HEAD):
        cut = slice(h * HEAD, (h + 1) * HEAD)
        query[:, cut] = spin(projected[:, cut], cosine[...], sine[...]).astype(bf16)


def key_value_body(normed, cosine, sine, *rest):
    weights, (keys, values) = rest[:8], rest[8:]
    place = position()
    projected = pieces_product(place, normed, weights, lambda w: w[0])
    for h in range(projected.shape[1] // HEAD):
        cut = slice(h * HEAD, (h + 1) * HEAD)
        keys[:, cut] = spin(projected[:, cut], cosine[...], sine[...]).astype(bf16)
    values[...] = pieces_product(place, normed, weights, lambda w: w[1]).astype(bf16)


def split_in_three(x):
    high = x.astype(bf16).astype(f32)
    middle = (x - high).astype(bf16).astype(f32)
    return high, middle, x - high - middle


def soft_weights(scores, live):
    scores = jnp.where(live, scores, FLOOR)
    most = jnp.max(scores, axis=-1, keepdims=True)
    weights = jnp.where(live, jnp.exp(scores - most), 0.0)
    return weights, most, jnp.sum(weights, axis=-1, keepdims=True)


def history_body(step, lengths, stack, k_cache, v_cache, out, scores, weights):
    meetings, span = k_cache.shape[0], k_cache.shape[1]
    place = position()
    rows = stack.shape[1]
    new = rows // meetings
    heads = 2 * SIDE
    starts = []
    for k in range(SIDE):
        block = SIDE * ((place[2] + SIDE - k) % SIDE) + (place[3] + SIDE - step) % SIDE
        for h in range(2):
            starts.append(pl.multiple_of(block * 256 + h * HEAD, HEAD))
    for i, start in enumerate(starts):
        cut = slice(i % 2 * HEAD, (i % 2 + 1) * HEAD)
        for m in range(meetings):
            here = slice(m * new, (m + 1) * new)
            scores[i, here, :] = matmul_t(
                stack[i // 2, here, cut], k_cache[m, :, pl.ds(start, HEAD)]
            )
    first = (place[2] * SIDE + place[3]) * span
    spot = first + lax.broadcasted_iota(jnp.int32, (rows, span), 1)
    upper = lax.broadcasted_iota(jnp.int32, (rows, span), 0) < new
    live = spot < jnp.where(upper, lengths[0], lengths[1])
    lane = lax.broadcasted_iota(jnp.int32, (rows, HEAD), 1)
    stats = jnp.zeros((rows, HEAD), f32)
    for i in range(heads):
        weight, most, total = soft_weights(scores[i] * HEAD**-0.5, live)
        weights[i] = weight.astype(bf16)
        stats = jnp.where(lane == i, most, jnp.where(lane == heads + i, total, stats))
    for i, start in enumerate(starts):
        for m in range(meetings):
            here = slice(m * new, (m + 1) * new)
            at = i * rows + m * new
            out[at : at + new, :] = matmul(
                weights[i, here, :], v_cache[m, :, pl.ds(start, HEAD)]
            ).astype(bf16)
    turned = jnp.transpose(stats)[: 2 * heads]
    base = heads * rows
    for n, piece in enumerate(split_in_three(turned)):
        out[base + 16 * n : base + 16 * n + 16, :] = piece.astype(bf16)


def turned_columns(pieces, rows):
    used = sum(p.shape[0] for p in pieces)
    fill = [jnp.zeros((rows - used, pieces[0].shape[1]), f32)] if rows > used else []
    return jnp.transpose(jnp.concatenate(list(pieces) + fill, axis=0))


def row_mix_body(p0, p1, p2, p3, own, o1, o2, o3):
    parts = (p0, p1, p2, p3)
    outs = (own, o1, o2, o3)
    heads = 2 * SIDE
    rows = p0.shape[1]
    base = heads * rows
    tops, totals = [], []
    for p in parts:
        tail = p[base : base + 48, :].astype(f32)
        stats = tail[:16] + tail[16:32] + tail[32:]
        tops.append(stats[:heads])
        totals.append(stats[heads:])
    top = jnp.maximum(jnp.maximum(tops[0], tops[1]), jnp.maximum(tops[2], tops[3]))
    factors = [jnp.exp(t - top) for t in tops]
    total = sum(t * f for t, f in zip(totals, factors))
    columns = turned_columns(factors, rows)
    for h in range(heads):
        cut = slice(h * rows, (h + 1) * rows)
        mixed = None
        for i, p in enumerate(parts):
            at = i * heads + h
            term = p[cut, :].astype(f32) * columns[:, at : at + 1]
            mixed = term if mixed is None else mixed + term
        outs[h // 2][(h % 2) * rows : (h % 2 + 1) * rows, :] = mixed.astype(bf16)
    spread = [piece for pair in zip(split_in_three(top), split_in_three(total)) for piece in pair]
    for k in range(SIDE):
        cut = slice(2 * k, 2 * k + 2)
        outs[k][2 * rows : 2 * rows + 16, :] = jnp.concatenate(
            [piece[cut] for piece in spread] + [jnp.zeros((4, rows), f32)], axis=0
        ).astype(bf16)


def new_part_body(query, keys, values, numer, stats_out):
    rows = query.shape[0]
    new = rows // 2
    causal = lax.broadcasted_iota(jnp.int32, (new, new), 0) >= lax.broadcasted_iota(
        jnp.int32, (new, new), 1
    )
    lane = lax.broadcasted_iota(jnp.int32, (new, HEAD), 1)
    stats = []
    for m in range(2):
        here = slice(m * new, (m + 1) * new)
        tile = jnp.zeros((new, HEAD), f32)
        for h in range(2):
            cut = slice(h * HEAD, (h + 1) * HEAD)
            weight, most, total = soft_weights(
                matmul_t(query[here, cut], keys[here, cut]) * HEAD**-0.5, causal
            )
            numer[h * rows + m * new : h * rows + (m + 1) * new, :] = matmul(
                weight.astype(bf16), values[here, cut]
            )
            tile = jnp.where(lane == h, most, jnp.where(lane == 2 + h, total, tile))
        stats.append(tile)
    stats_out[...] = jnp.transpose(jnp.concatenate(stats, axis=0))[:8]


def final_mix_body(p0, p1, p2, p3, numer, new_stats, out):
    parts = (p0, p1, p2, p3)
    rows = numer.shape[0] // 2
    tops, totals = [], []
    for p in parts:
        tail = p[2 * rows : 2 * rows + 16, :].astype(f32)
        tops.append(tail[0:2] + tail[4:6] + tail[8:10])
        totals.append(tail[2:4] + tail[6:8] + tail[10:12])
    tops.append(new_stats[0:2])
    totals.append(new_stats[2:4])
    top = tops[0]
    for t in tops[1:]:
        top = jnp.maximum(top, t)
    factors = [jnp.exp(t - top) for t in tops]
    total = sum(t * f for t, f in zip(totals, factors))
    columns = turned_columns([f / total for f in factors], rows)
    for h in range(2):
        cut = slice(h * rows, (h + 1) * rows)
        mixed = numer[cut, :] * columns[:, 8 + h : 9 + h]
        for i, p in enumerate(parts):
            mixed = mixed + p[cut, :].astype(f32) * columns[:, 2 * i + h : 2 * i + h + 1]
        out[:, h * HEAD : (h + 1) * HEAD] = mixed.astype(bf16)


def project_body(a0, a1, a2, a3, *rest):
    weights, (own, o1, o2, o3, across, sums) = rest[:8], rest[8:]
    place = position()
    for k, a in enumerate((a0, a1, a2, a3)):
        across[(place[2] + SIDE - k) % SIDE] = a[...]
    for c in range(2):
        total = None
        for j in range(SIDE):
            part = matmul(across[(place[0] + SIDE - j) % SIDE], weights[2 * j + c][...])
            total = part if total is None else total + part
        first = 2 * ((place[1] + c) % 2)
        sums[first] = total[:, :256]
        sums[first + 1] = total[:, 256:]
    own[...] = sums[place[3]]
    for j, o in enumerate((o1, o2, o3)):
        o[...] = sums[(place[3] + j + 1) % SIDE].astype(bf16)


def total_body(own, g1, g2, g3, out):
    out[...] = (
        own[...] + g1[...].astype(f32) + g2[...].astype(f32) + g3[...].astype(f32)
    ).astype(bf16)


def layer(
    frames,
    span_source,
    adapter_weight,
    adapter_bias,
    norm_gain,
    qkv_weight,
    out_weight,
    k_cache,
    v_cache,
    lengths,
):
    rows = frames.shape[0]
    cols = adapter_weight.shape[1]
    meetings = lengths.shape[0]
    new = rows // meetings
    heads = 2 * SIDE
    by_kind = jnp.transpose(qkv_weight, (1, 0, 2))
    feats = by_kind.shape[1]
    longest = SIDE * SIDE * k_cache.shape[1]
    coarse = jnp.asarray(turns(longest // new + 8, new))
    fine = jnp.asarray(turns(2 * new, 1))
    adapted, query_weight, other_weight, cosine, sine = kernel_call(
        adapter_body,
        [
            (SMEM, span_source),
            (SMEM, lengths),
            (WHOLE, frames),
            (WHOLE, adapter_weight),
            (WHOLE, adapter_bias.reshape(1, cols)),
            (WHOLE, coarse),
            (WHOLE, fine),
            (ANY, by_kind),
        ],
        (
            near((rows, cols), bf16),
            near((feats, cols), bf16),
            near((2, feats, cols), bf16),
            near((rows, HEAD), f32),
            near((rows, HEAD), f32),
        ),
        [pltpu.VMEM(frames.shape, bf16), pltpu.SemaphoreType.DMA((2,))],
    )
    column = stacked(from_ring(adapted, y_shift))
    stacks = from_ring(column, z_shift)

    query_weights = over_x(query_weight)
    other_weights = over_x(other_weight)
    swapped = swap_xy(out_weight)
    out_weights = over_x(swapped)

    gain = norm_gain.reshape(SIDE * SIDE, 1, cols)
    query, normed = kernel_call(
        query_body,
        [(VMEM, s) for s in stacks]
        + [(VMEM, gain), (VMEM, cosine), (VMEM, sine)]
        + [(VMEM, w) for w in query_weights],
        (
            near((rows, cols), bf16),
            near((SIDE * SIDE, rows, cols), bf16),
        ),
    )
    query_column = stacked(from_ring(query, y_shift))
    query_stacks = from_ring(query_column, z_shift)

    keys, values = kernel_call(
        key_value_body,
        [(VMEM, normed), (VMEM, cosine), (VMEM, sine)]
        + [(VMEM, w) for w in other_weights],
        (near((rows, cols), bf16), near((rows, cols), bf16)),
    )

    def history(step):
        return kernel_call(
            lambda *refs: history_body(step, *refs),
            [
                (SMEM, lengths),
                (VMEM, query_stacks[step]),
                (VMEM, k_cache),
                (VMEM, v_cache),
            ],
            near((heads * rows + 48, HEAD), bf16),
            [
                pltpu.VMEM((heads, rows, HEAD), f32),
                pltpu.VMEM((heads, rows, HEAD), bf16),
            ],
        )

    own = history(0)
    back = {}
    for j in ORDER:
        part = history(j)
        back[j] = z_shift(part, -j)
    block = near((2 * rows + 16, HEAD), bf16)
    mixed = kernel_call(
        row_mix_body,
        [(VMEM, p) for p in (own, back[1], back[2], back[3])],
        (block, block, block, block),
    )
    returned = {k: y_shift(mixed[k], -k) for k in ORDER}
    numer, new_stats = kernel_call(
        new_part_body,
        [(VMEM, query), (VMEM, keys), (VMEM, values)],
        (near((2 * rows, HEAD), f32), near((8, rows), f32)),
    )
    attended = kernel_call(
        final_mix_body,
        [(VMEM, p) for p in (mixed[0], returned[1], returned[2], returned[3], numer, new_stats)],
        near((rows, cols), bf16),
    )
    across = from_ring(attended, y_shift)
    part = near((rows, cols), bf16)
    sums = kernel_call(
        project_body,
        [(VMEM, a) for a in across] + [(VMEM, w) for w in out_weights],
        (near((rows, cols), f32), part, part, part),
        [pltpu.VMEM((SIDE, rows, cols), bf16), pltpu.VMEM((SIDE, rows, cols), f32)],
    )
    got = [z_shift(sums[j], j) for j in ORDER]
    attn_out = kernel_call(
        total_body, [(VMEM, p) for p in (sums[0], *got)], far((rows, cols), bf16)
    )
    return attn_out, keys, values


def solution(mesh):
    return jax.shard_map(
        layer,
        mesh=mesh,
        in_specs=(
            P("wt", None),
            P("wt"),
            P(None, "ctx"),
            P("ctx"),
            P(),
            P("wt", None, "ctx"),
            P("ctx", "wt"),
            P("wt", "ctx", None),
            P("wt", "ctx", None),
            P("wt"),
        ),
        out_specs=(P("wt", "ctx"), P("wt", "ctx"), P("wt", "ctx")),
        check_vma=False,
    )
```

```python
import jax
import jax.numpy as jnp
import numpy as np
from jax import lax
from jax.experimental import pallas as pl
from jax.experimental.pallas import tpu as pltpu
from jax.sharding import PartitionSpec as P


HEAD = 128
SIDE = 4
FLOOR = -1e30

bf16 = jnp.bfloat16
f32 = jnp.float32


def y_shift(x, k):
    pairs = [
        (y * SIDE + z, ((y + k) % SIDE) * SIDE + z) for y in range(SIDE) for z in range(SIDE)
    ]
    return lax.ppermute(x, "ctx", pairs)


def z_shift(x, k):
    pairs = [
        (y * SIDE + z, y * SIDE + (z + k) % SIDE) for y in range(SIDE) for z in range(SIDE)
    ]
    return lax.ppermute(x, "ctx", pairs)


def x_shift(x, k):
    pairs = [(2 * i + c, 2 * ((i + k) % SIDE) + c) for i in range(SIDE) for c in range(2)]
    return lax.ppermute(x, "wt", pairs)


def other_core(x):
    return lax.ppermute(x, "wt", [(i, i ^ 1) for i in range(2 * SIDE)])


def swap_xy(x):
    def place(i, y, z, c):
        return (y * SIDE + z) * 2 * SIDE + 2 * i + c

    pairs = [
        (place(i, y, z, c), place((i + y) % SIDE, i, z, c))
        for i in range(SIDE)
        for y in range(SIDE)
        for z in range(SIDE)
        for c in range(2)
    ]
    return lax.ppermute(x, ("ctx", "wt"), pairs)


ORDER = (1, 3, 2)


def from_ring(x, shift):
    got = {}
    for k in ORDER:
        got[k] = shift(x, k)
    return [x, got[1], got[2], got[3]]


def over_x(x):
    mine = from_ring(x, x_shift)
    both = []
    for m in mine:
        both += [m, other_core(m)]
    return both


VMEM = pl.BlockSpec(memory_space=pltpu.VMEM)
SMEM = pl.BlockSpec(memory_space=pltpu.SMEM)
ANY = pl.BlockSpec(memory_space=pl.ANY)
WHOLE = pl.BlockSpec()


def held(x):
    return pltpu.with_memory_space_constraint(x, pltpu.VMEM)


def outside(x):
    return pltpu.with_memory_space_constraint(x, pltpu.HBM)


def placed(spec, x):
    return held(x) if spec is VMEM else outside(x)


def kernel_call(body, ins, out_shape, scratch=(), limit=12):
    single = not isinstance(out_shape, tuple)
    return pl.pallas_call(
        body,
        in_specs=[s for s, _ in ins],
        out_specs=VMEM if single else tuple(VMEM for _ in out_shape),
        out_shape=out_shape,
        scratch_shapes=list(scratch),
        compiler_params=pltpu.CompilerParams(vmem_limit_bytes=limit << 20),
    )(*[placed(s, a) for s, a in ins])


def near(dims, kind):
    return pltpu.VMEM(dims, kind)


def far(dims, kind):
    return jax.ShapeDtypeStruct(dims, kind)


def position():
    ctx_rank = lax.axis_index("ctx")
    wt_rank = lax.axis_index("wt")
    return wt_rank // 2, wt_rank % 2, ctx_rank // SIDE, ctx_rank % SIDE


def matmul(a, b):
    return jnp.dot(a, b, preferred_element_type=f32)


def matmul_t(a, b):
    return lax.dot_general(a, b, (((1,), (1,)), ((), ())), preferred_element_type=f32)


def turns(count, step):
    freq = 10000.0 ** (-2.0 * (np.arange(HEAD) % (HEAD // 2)) / HEAD)
    angle = step * np.arange(count)[:, None] * freq[None, :]
    return np.stack([np.cos(angle), np.sin(angle)]).astype(np.float32)


def rope_tables(lengths, coarse, fine, cosine, sine, new):
    lane = lax.broadcasted_iota(jnp.int32, (new, HEAD), 1)
    for m in range(cosine.shape[0] // new):
        high = lengths[m] // new
        low = lengths[m] - high * new
        c1, s1 = coarse[0, pl.ds(high, 1), :], coarse[1, pl.ds(high, 1), :]
        c2, s2 = fine[0, pl.ds(low, new), :], fine[1, pl.ds(low, new), :]
        here = slice(m * new, (m + 1) * new)
        cosine[here, :] = c1 * c2 - s1 * s2
        value = s1 * c2 + c1 * s2
        sine[here, :] = jnp.where(lane < HEAD // 2, -value, value)


def adapter_body(
    source,
    lengths,
    frames,
    weight,
    bias,
    coarse,
    fine,
    kinds,
    out,
    query_weight,
    other_weight,
    cosine,
    sine,
    ordered,
    sems,
):
    copies = (
        pltpu.make_async_copy(kinds.at[0], query_weight, sems.at[0]),
        pltpu.make_async_copy(kinds.at[1:3], other_weight, sems.at[1]),
    )
    for copy in copies:
        copy.start()
    rope_tables(lengths, coarse, fine, cosine, sine, fine.shape[1] // 2)
    spans = source.shape[0]
    rows = frames.shape[0] // spans
    for g in range(spans):
        start = pl.multiple_of(source[g] * rows, rows)
        ordered[g * rows : (g + 1) * rows, :] = frames[pl.ds(start, rows), :]
    out[...] = (matmul(ordered[...], weight[...]) + bias[...]).astype(bf16)
    for copy in copies:
        copy.wait()


def stack_body(a0, a1, a2, a3, out):
    for k, a in enumerate((a0, a1, a2, a3)):
        out[k] = a[...]


def stacked(parts):
    dims = (SIDE, *parts[0].shape)
    return kernel_call(stack_body, [(VMEM, p) for p in parts], near(dims, bf16))


def spin(u, cosine, sine):
    return u * cosine + pltpu.roll(u, HEAD // 2, 1) * sine


def pieces_product(place, normed, weights, take):
    total = None
    for n, weight in enumerate(weights):
        shard = 2 * ((place[0] + SIDE - n // 2) % SIDE) + (place[1] + n) % 2
        w = take(weight)
        half = w.shape[0] // 2
        part = matmul(normed[2 * shard], w[:half]) + matmul(normed[2 * shard + 1], w[half:])
        total = part if total is None else total + part
    return total


def query_body(s0, s1, s2, s3, gain, cosine, sine, *rest):
    weights, (query, turned, normed) = rest[:8], rest[8:]
    place = position()
    stacks = (s0, s1, s2, s3)
    rows = s0.shape[1]
    sums = jnp.zeros((rows, HEAD), f32)
    for stack in stacks:
        for k in range(SIDE):
            wide = stack[k].astype(f32)
            square = wide * wide
            sums = sums + (square[:, :HEAD] + square[:, HEAD:])
    width = SIDE * SIDE * s0.shape[2]
    factor = lax.rsqrt(jnp.sum(sums, axis=-1, keepdims=True) * (1.0 / width) + 1e-06)
    for j, stack in enumerate(stacks):
        for k in range(SIDE):
            block = SIDE * ((place[2] + SIDE - k) % SIDE) + (place[3] + SIDE - j) % SIDE
            normed[block] = (stack[k].astype(f32) * factor * gain[block]).astype(bf16)
    projected = pieces_product(place, normed, weights, lambda w: w[...])
    for h in range(projected.shape[1] // HEAD):
        cut = slice(h * HEAD, (h + 1) * HEAD)
        head = spin(projected[:, cut], cosine[...], sine[...])
        query[:, cut] = head.astype(bf16)
        turned[cut, :] = jnp.transpose(head).astype(bf16)


def key_value_body(normed, cosine, sine, *rest):
    weights, (keys, values) = rest[:8], rest[8:]
    place = position()
    projected = pieces_product(place, normed, weights, lambda w: w[0])
    for h in range(projected.shape[1] // HEAD):
        cut = slice(h * HEAD, (h + 1) * HEAD)
        keys[:, cut] = spin(projected[:, cut], cosine[...], sine[...]).astype(bf16)
    values[...] = pieces_product(place, normed, weights, lambda w: w[1]).astype(bf16)


def split_in_three(x):
    high = x.astype(bf16).astype(f32)
    middle = (x - high).astype(bf16).astype(f32)
    return high, middle, x - high - middle


def soft_weights(scores, live):
    scores = jnp.where(live, scores, FLOOR)
    most = jnp.max(scores, axis=-1, keepdims=True)
    weights = jnp.where(live, jnp.exp(scores - most), 0.0)
    return weights, most, jnp.sum(weights, axis=-1, keepdims=True)


def history_body(step, lengths, stack, k_cache, v_cache, out, scores, weights):
    meetings, span = k_cache.shape[0], k_cache.shape[1]
    place = position()
    rows = stack.shape[2]
    new = rows // meetings
    heads = 2 * SIDE
    starts = []
    for k in range(SIDE):
        block = SIDE * ((place[2] + SIDE - k) % SIDE) + (place[3] + SIDE - step) % SIDE
        for h in range(2):
            starts.append(pl.multiple_of(block * 256 + h * HEAD, HEAD))
    early = lax.broadcasted_iota(jnp.int32, (span, rows), 1) < new
    first = (place[2] * SIDE + place[3]) * span
    spot = first + lax.broadcasted_iota(jnp.int32, (span, rows), 0)
    live = spot < jnp.where(early, lengths[0], lengths[1])
    for i, start in enumerate(starts):
        query = stack[i // 2, i % 2 * HEAD : (i % 2 + 1) * HEAD, :]
        both = [matmul(k_cache[m, :, pl.ds(start, HEAD)], query) for m in range(meetings)]
        scores[i] = jnp.where(early, both[0], both[1])
    tops, totals = [], []
    for i in range(heads):
        score = jnp.where(live, scores[i] * HEAD**-0.5, FLOOR)
        most = jnp.max(score, axis=0, keepdims=True)
        weight = jnp.exp(score - jnp.where(most > 0.5 * FLOOR, most, 0.0))
        tops.append(most)
        totals.append(jnp.sum(weight, axis=0, keepdims=True))
        weights[i] = jnp.transpose(weight.astype(bf16))
    for i, start in enumerate(starts):
        for m in range(meetings):
            here = slice(m * new, (m + 1) * new)
            at = i * rows + m * new
            out[at : at + new, :] = matmul(
                weights[i, here, :], v_cache[m, :, pl.ds(start, HEAD)]
            ).astype(bf16)
    stats = jnp.concatenate(tops + totals, axis=0)
    base = heads * rows
    for n, piece in enumerate(split_in_three(stats)):
        out[base + 16 * n : base + 16 * n + 16, :] = piece.astype(bf16)


def turned_columns(pieces, rows):
    used = sum(p.shape[0] for p in pieces)
    fill = [jnp.zeros((rows - used, pieces[0].shape[1]), f32)] if rows > used else []
    return jnp.transpose(jnp.concatenate(list(pieces) + fill, axis=0))


def row_mix_body(p0, p1, p2, p3, own, o1, o2, o3):
    parts = (p0, p1, p2, p3)
    outs = (own, o1, o2, o3)
    heads = 2 * SIDE
    rows = p0.shape[1]
    base = heads * rows
    tops, totals = [], []
    for p in parts:
        tail = p[base : base + 48, :].astype(f32)
        stats = tail[:16] + tail[16:32] + tail[32:]
        tops.append(stats[:heads])
        totals.append(stats[heads:])
    top = jnp.maximum(jnp.maximum(tops[0], tops[1]), jnp.maximum(tops[2], tops[3]))
    factors = [jnp.exp(t - top) for t in tops]
    total = sum(t * f for t, f in zip(totals, factors))
    columns = turned_columns(factors, rows)
    for h in range(heads):
        cut = slice(h * rows, (h + 1) * rows)
        mixed = None
        for i, p in enumerate(parts):
            at = i * heads + h
            term = p[cut, :].astype(f32) * columns[:, at : at + 1]
            mixed = term if mixed is None else mixed + term
        outs[h // 2][(h % 2) * rows : (h % 2 + 1) * rows, :] = mixed.astype(bf16)
    spread = [piece for pair in zip(split_in_three(top), split_in_three(total)) for piece in pair]
    for k in range(SIDE):
        cut = slice(2 * k, 2 * k + 2)
        outs[k][2 * rows : 2 * rows + 16, :] = jnp.concatenate(
            [piece[cut] for piece in spread] + [jnp.zeros((4, rows), f32)], axis=0
        ).astype(bf16)


def new_part_body(query, keys, values, numer, stats_out):
    rows = query.shape[0]
    new = rows // 2
    causal = lax.broadcasted_iota(jnp.int32, (new, new), 0) >= lax.broadcasted_iota(
        jnp.int32, (new, new), 1
    )
    lane = lax.broadcasted_iota(jnp.int32, (new, HEAD), 1)
    stats = []
    for m in range(2):
        here = slice(m * new, (m + 1) * new)
        tile = jnp.zeros((new, HEAD), f32)
        for h in range(2):
            cut = slice(h * HEAD, (h + 1) * HEAD)
            weight, most, total = soft_weights(
                matmul_t(query[here, cut], keys[here, cut]) * HEAD**-0.5, causal
            )
            numer[h * rows + m * new : h * rows + (m + 1) * new, :] = matmul(
                weight.astype(bf16), values[here, cut]
            )
            tile = jnp.where(lane == h, most, jnp.where(lane == 2 + h, total, tile))
        stats.append(tile)
    stats_out[...] = jnp.transpose(jnp.concatenate(stats, axis=0))[:8]


def final_mix_body(p0, p1, p2, p3, numer, new_stats, out):
    parts = (p0, p1, p2, p3)
    rows = numer.shape[0] // 2
    tops, totals = [], []
    for p in parts:
        tail = p[2 * rows : 2 * rows + 16, :].astype(f32)
        tops.append(tail[0:2] + tail[4:6] + tail[8:10])
        totals.append(tail[2:4] + tail[6:8] + tail[10:12])
    tops.append(new_stats[0:2])
    totals.append(new_stats[2:4])
    top = tops[0]
    for t in tops[1:]:
        top = jnp.maximum(top, t)
    factors = [jnp.exp(t - top) for t in tops]
    total = sum(t * f for t, f in zip(totals, factors))
    columns = turned_columns([f / total for f in factors], rows)
    for h in range(2):
        cut = slice(h * rows, (h + 1) * rows)
        mixed = numer[cut, :] * columns[:, 8 + h : 9 + h]
        for i, p in enumerate(parts):
            mixed = mixed + p[cut, :].astype(f32) * columns[:, 2 * i + h : 2 * i + h + 1]
        out[:, h * HEAD : (h + 1) * HEAD] = mixed.astype(bf16)


def project_body(a0, a1, a2, a3, *rest):
    weights, (own, o1, o2, o3, across, sums) = rest[:8], rest[8:]
    place = position()
    for k, a in enumerate((a0, a1, a2, a3)):
        across[(place[2] + SIDE - k) % SIDE] = a[...]
    for c in range(2):
        total = None
        for j in range(SIDE):
            part = matmul(across[(place[0] + 2 * SIDE - place[2] - j) % SIDE], weights[2 * j + c][...])
            total = part if total is None else total + part
        first = 2 * ((place[1] + c) % 2)
        sums[first] = total[:, :256]
        sums[first + 1] = total[:, 256:]
    own[...] = sums[place[3]]
    for j, o in enumerate((o1, o2, o3)):
        o[...] = sums[(place[3] + j + 1) % SIDE].astype(bf16)


def total_body(own, g1, g2, g3, out):
    out[...] = (
        own[...] + g1[...].astype(f32) + g2[...].astype(f32) + g3[...].astype(f32)
    ).astype(bf16)


def layer(
    frames,
    span_source,
    adapter_weight,
    adapter_bias,
    norm_gain,
    qkv_weight,
    out_weight,
    k_cache,
    v_cache,
    lengths,
):
    rows = frames.shape[0]
    cols = adapter_weight.shape[1]
    meetings = lengths.shape[0]
    new = rows // meetings
    heads = 2 * SIDE
    by_kind = jnp.transpose(qkv_weight, (1, 0, 2))
    feats = by_kind.shape[1]
    longest = SIDE * SIDE * k_cache.shape[1]
    coarse = jnp.asarray(turns(longest // new + 8, new))
    fine = jnp.asarray(turns(2 * new, 1))
    adapted, query_weight, other_weight, cosine, sine = kernel_call(
        adapter_body,
        [
            (SMEM, span_source),
            (SMEM, lengths),
            (WHOLE, frames),
            (WHOLE, adapter_weight),
            (WHOLE, adapter_bias.reshape(1, cols)),
            (WHOLE, coarse),
            (WHOLE, fine),
            (ANY, by_kind),
        ],
        (
            near((rows, cols), bf16),
            near((feats, cols), bf16),
            near((2, feats, cols), bf16),
            near((rows, HEAD), f32),
            near((rows, HEAD), f32),
        ),
        [pltpu.VMEM(frames.shape, bf16), pltpu.SemaphoreType.DMA((2,))],
    )
    column = stacked(from_ring(adapted, y_shift))
    stacks = from_ring(column, z_shift)

    query_weights = over_x(query_weight)
    other_weights = over_x(other_weight)
    swapped = swap_xy(out_weight)
    out_weights = over_x(swapped)

    gain = norm_gain.reshape(SIDE * SIDE, 1, cols)
    query, query_turned, normed = kernel_call(
        query_body,
        [(VMEM, s) for s in stacks]
        + [(VMEM, gain), (VMEM, cosine), (VMEM, sine)]
        + [(VMEM, w) for w in query_weights],
        (
            near((rows, cols), bf16),
            near((cols, rows), bf16),
            near((SIDE * SIDE, rows, cols), bf16),
        ),
    )
    query_column = stacked(from_ring(query_turned, y_shift))
    query_stacks = from_ring(query_column, z_shift)

    keys, values = kernel_call(
        key_value_body,
        [(VMEM, normed), (VMEM, cosine), (VMEM, sine)]
        + [(VMEM, w) for w in other_weights],
        (near((rows, cols), bf16), near((rows, cols), bf16)),
    )

    def history(step):
        return kernel_call(
            lambda *refs: history_body(step, *refs),
            [
                (SMEM, lengths),
                (VMEM, query_stacks[step]),
                (VMEM, k_cache),
                (VMEM, v_cache),
            ],
            near((heads * rows + 48, HEAD), bf16),
            [
                pltpu.VMEM((heads, rows, HEAD), f32),
                pltpu.VMEM((heads, rows, HEAD), bf16),
            ],
        )

    own = history(0)
    back = {}
    for j in ORDER:
        part = history(j)
        back[j] = z_shift(part, -j)
    block = near((2 * rows + 16, HEAD), bf16)
    mixed = kernel_call(
        row_mix_body,
        [(VMEM, p) for p in (own, back[1], back[2], back[3])],
        (block, block, block, block),
    )
    returned = {k: y_shift(mixed[k], -k) for k in ORDER}
    numer, new_stats = kernel_call(
        new_part_body,
        [(VMEM, query), (VMEM, keys), (VMEM, values)],
        (near((2 * rows, HEAD), f32), near((8, rows), f32)),
    )
    attended = kernel_call(
        final_mix_body,
        [(VMEM, p) for p in (mixed[0], returned[1], returned[2], returned[3], numer, new_stats)],
        near((rows, cols), bf16),
    )
    across = from_ring(attended, y_shift)
    part = near((rows, cols), bf16)
    sums = kernel_call(
        project_body,
        [(VMEM, a) for a in across] + [(VMEM, w) for w in out_weights],
        (near((rows, cols), f32), part, part, part),
        [pltpu.VMEM((SIDE, rows, cols), bf16), pltpu.VMEM((SIDE, rows, cols), f32)],
    )
    got = [z_shift(sums[j], j) for j in ORDER]
    attn_out = kernel_call(
        total_body, [(VMEM, p) for p in (sums[0], *got)], far((rows, cols), bf16)
    )
    return attn_out, keys, values


def solution(mesh):
    return jax.shard_map(
        layer,
        mesh=mesh,
        in_specs=(
            P("wt", None),
            P("wt"),
            P(None, "ctx"),
            P("ctx"),
            P(),
            P("wt", None, "ctx"),
            P("ctx", "wt"),
            P("wt", "ctx", None),
            P("wt", "ctx", None),
            P("wt"),
        ),
        out_specs=(P("wt", "ctx"), P("wt", "ctx"), P("wt", "ctx")),
        check_vma=False,
    )
```
